32 devices in a mesh: dp: 2 (over core), ctx: 16 (over z, y, x).
Axes of the slice: x: 2, y: 2, z: 4, core: 2. Of those that a mesh axis runs over, the one named last changes fastest.
Arguments:
- tokens: bfloat16 [4, 1024, 2048], P('dp', 'ctx'), may hold values from -6 to 6
- segment_ids: int32 [4, 1024], P('dp'), may hold values from 0 to 7, never falling along the last dimension, each value on 1 to 512 neighbouring positions
- routes: int32 [4, 1024, 8], P('dp', 'ctx'), may hold values from 0 to 15, all different within a row
- cotangent: bfloat16 [4, 1024, 2048], P('dp', 'ctx'), may hold values from -6 to 6
- q_weight: bfloat16 [2048, 4096], P(('dp', 'ctx')), may hold values from -0.125 to 0.125
- k_weight: bfloat16 [2048, 512], P(('dp', 'ctx')), may hold values from -0.125 to 0.125
- v_weight: bfloat16 [2048, 512], P(('dp', 'ctx')), may hold values from -0.125 to 0.125
- o_weight: bfloat16 [4096, 2048], P(('dp', 'ctx')), may hold values from -0.375 to 0.375
- router_weight: bfloat16 [2048, 16], P(('dp', 'ctx')), may hold values from -0.0625 to 0.0625
- norm_gains: bfloat16 [4352], P(('dp', 'ctx')), may hold values from 0.25 to 1.75
- gate_up_weight: bfloat16 [16, 2048, 1536], P('ctx', 'dp'), may hold values from -0.125 to 0.125
- down_weight: bfloat16 [16, 768, 2048], P('ctx', None, 'dp'), may hold values from -0.875 to 0.875
Outputs:
- output: bfloat16 [4, 1024, 2048], P('dp', 'ctx')
- input_grad: bfloat16 [4, 1024, 2048], P('dp', 'ctx')
- q_weight_grad: float32 [2048, 4096], P(('dp', 'ctx'))
- k_weight_grad: float32 [2048, 512], P(('dp', 'ctx'))
- v_weight_grad: float32 [2048, 512], P(('dp', 'ctx'))
- o_weight_grad: float32 [4096, 2048], P(('dp', 'ctx'))
- router_weight_grad: float32 [2048, 16], P(('dp', 'ctx'))
- norm_gains_grad: float32 [4352], P(('dp', 'ctx'))
- gate_up_weight_grad: float32 [16, 2048, 1536], P('ctx', 'dp')
- down_weight_grad: float32 [16, 768, 2048], P('ctx', None, 'dp')
The draws below stay inside these ranges and needn't reach their ends.
Inputs may be any that keep to these rules, and one draw needn't show every extreme that they name: `segment_ids`: Non-decreasing along each sequence; every document holds at most 512 positions, and one holds exactly that many. `routes`: each token names 8 different experts; every expert is named by some token.
All inputs are finite; a program needn't handle non-finite values.
Results may differ from the reference program's by a relative error of at most 0.019.
Values may be sent and summed in bfloat16 or wider, within the bound.
No kernel may reach another device: no remote copies, remote signals or barrier semaphores. Data moves between devices by JAX's collectives and lax.ppermute only.
A program may use at most 320 MiB of HBM per device.

```python
import math
import jax
import jax.numpy as jnp
import numpy as np
from jax import lax

D = 2048
H = 32
KV = 4
HD = 128
FF = 768
TOPK = 8
DOCS = 8
SEQS = 4
LEN = 1024
BLOCK = 64
EXPERTS = 16
CAP = 40
N_CTX = 16


def steps_of(own_key, dims, split, low, high):
    factor_of, own = 1.0, jax.random.fold_in(own_key, 6)
    for dim, shards_of in split:
        draws = jnp.exp(jax.random.uniform(jax.random.fold_in(own, dim), (shards_of,), jnp.float32, low / len(split), high / len(split)))
        factor_of = factor_of * jnp.repeat(draws, dims[dim] // shards_of).reshape([-1 if axis == dim else 1 for axis in range(len(dims))])
    return factor_of


def picks_of(own_key, rows, number_of, top, lift):
    sequence = jax.random.permutation(jax.random.fold_in(own_key, 1), number_of)
    favour = sequence
    for power in range(3):
        favour = favour * favour // number_of
    favour = favour * lift // number_of
    lots = jax.random.randint(jax.random.fold_in(own_key, 2), (rows, number_of), 0, 4096) + favour
    fixed_rows = jax.random.permutation(jax.random.fold_in(own_key, 3), rows)[jnp.arange(number_of) % rows]
    lots = jnp.where(jnp.arange(rows)[:, None] == fixed_rows[None, :], 1 << 14, lots)
    score = lots * number_of + jnp.arange(number_of)
    return lax.top_k(score.astype(jnp.int32), top)[1].astype(jnp.int32)


def profile(amount, total, limit, slope):
    loads = [(1 << 20) // math.isqrt(standing ** slope) + 1 for standing in range(2, amount + 1)]
    surplus, counts = total - limit - (amount - 1), [1] * (amount - 1)
    while surplus > 0:
        candidates = [i for i in range(amount - 1) if counts[i] < limit]
        mass, remaining = sum([loads[i] for i in candidates]), surplus
        for i in candidates:
            addition = min(limit - counts[i], max(1, remaining * loads[i] // mass), surplus)
            counts[i] = counts[i] + addition
            surplus = surplus - addition
    return np.array([limit] + counts)


def ragged(stream_key, count, total, most, slope):
    if count == 2:
        one = jax.random.randint(stream_key, (), max(1, total - most), min(most, total - 1) + 1)
        return jnp.stack([one, total - one])
    sizes = jnp.asarray(profile(count, total, most, slope), jnp.int32)
    pairs = (count - 1) // 2
    giver, sink = sizes[1:1 + 2 * pairs:2], sizes[2:2 + 2 * pairs:2]
    room = jnp.minimum(giver - 1, most - sink)
    shifted = jax.random.randint(jax.random.fold_in(stream_key, 1), (pairs,), 0, 1 << 20) % (room + 1)
    sizes = sizes.at[1:1 + 2 * pairs:2].set(giver - shifted).at[2:2 + 2 * pairs:2].set(sink + shifted)
    return sizes[jax.random.permutation(jax.random.fold_in(stream_key, 2), count)]


def scatter_about(key, shape, width, most, cuts=(), held_as=jnp.bfloat16):
    array = width * jax.random.normal(key, shape, jnp.float32)
    if cuts:
        array = array * steps_of(key, shape, cuts, -0.22, 0.18)
    return jnp.clip(array, -most, most).astype(held_as)


def setup_inputs(seed: int = 0) -> dict:
    key_list = jax.random.split(jax.random.key(seed), 13)
    return {
        "tokens": scatter_about(key_list[0], (SEQS, LEN, D), 1.0, 6.0, ((0, 2), (1, 16))),
        "segment_ids": jax.vmap(lambda own: jnp.searchsorted(jnp.cumsum(ragged(own, DOCS, LEN, LEN // 2, 2)), jnp.arange(LEN), side="right"))(jax.random.split(key_list[1], SEQS)).reshape((SEQS, LEN)).astype(jnp.int32),
        "routes": picks_of(key_list[2], SEQS * LEN, EXPERTS, TOPK, 4096).reshape((SEQS, LEN, TOPK)),
        "cotangent": scatter_about(key_list[3], (SEQS, LEN, D), 1.0, 6.0, ((0, 2), (1, 16))),
        "q_weight": scatter_about(key_list[4], (D, H * HD), D ** -0.5, 0.125, ((0, 32),)),
        "k_weight": scatter_about(key_list[5], (D, KV * HD), D ** -0.5, 0.125, ((0, 32),)),
        "v_weight": scatter_about(key_list[6], (D, KV * HD), D ** -0.5, 0.125, ((0, 32),)),
        "o_weight": scatter_about(key_list[7], (H * HD, D), (H * HD // 16) ** -0.5, 0.375, ((0, 32),)),
        "router_weight": scatter_about(key_list[8], (D, EXPERTS), (4 * D) ** -0.5, 0.0625, ((0, 32),)),
        "norm_gains": jnp.clip(1.0 + 0.15 * jax.random.normal(key_list[9], (2 * D + 2 * HD,), jnp.float32), 0.25, 1.75).astype(jnp.bfloat16),
        "gate_up_weight": scatter_about(key_list[10], (EXPERTS, D, 2 * FF), D ** -0.5, 0.125, ((0, 16), (1, 2))),
        "down_weight": scatter_about(key_list[11], (EXPERTS, FF, D), (FF // 16) ** -0.5, 0.875, ((0, 16), (2, 2))),
    }


@jax.custom_vjp
def low(v):
    return lax.optimization_barrier(v.astype(jnp.bfloat16)).astype(jnp.float32)

@jax.custom_vjp
def low_back(v):
    return v

def low_keep(v):
    return (low(v), None)

def low_pass(kept, grad):
    return (grad,)

def back_keep(v):
    return (v, None)

def back_low(kept, grad):
    return (low(grad),)
low.defvjp(low_keep, low_pass)
low_back.defvjp(back_keep, back_low)
eps_norm = 1e-06
rope_base = 1000000.0
neg_big = -1e+30
highest = lax.Precision.HIGHEST

def rms_scale(operand):
    return lax.rsqrt(lax.optimization_barrier(jnp.mean(operand * operand, axis=-1, keepdims=True)) + eps_norm)

def rotate(operand, cosine, sine_table):
    half_width = operand.shape[-1] // 2
    turned = jnp.concatenate([-operand[..., half_width:], operand[..., :half_width]], axis=-1)
    return operand * cosine + turned * sine_table

def rope_tables(positions):
    frequency = rope_base ** (-(jnp.arange(HD // 2, dtype=jnp.float32) * 2.0 / HD))
    angles = positions.astype(jnp.float32)[:, None] * frequency[None, :]
    angles = jnp.concatenate([angles, angles], axis=-1)
    return (jnp.cos(angles), jnp.sin(angles))

def layer(tokens, params, segments, routes, cosine, sine_table):
    q_weight, k_weight, v_weight, o_weight, router_weight, norm_gains, gate_up_weight, down_weight = params
    attn_gain = norm_gains[:D]
    ffn_gain = norm_gains[D:2 * D]
    q_gain = norm_gains[2 * D:2 * D + HD]
    k_gain = norm_gains[2 * D + HD:]
    groups = H // KV
    score_scale = HD ** (-0.5)
    normed = low(tokens * rms_scale(tokens) * attn_gain)
    q_proj = low_back(jnp.dot(normed, q_weight, precision=highest)).reshape(LEN, H, HD)
    k_proj = low_back(jnp.dot(normed, k_weight, precision=highest)).reshape(LEN, KV, HD)
    values = low(low_back(jnp.dot(normed, v_weight, precision=highest))).reshape(LEN, KV, HD)
    queries = low(rotate(q_proj * rms_scale(q_proj) * q_gain, cosine[:, None, :], sine_table[:, None, :]))
    key_rows = low(rotate(k_proj * rms_scale(k_proj) * k_gain, cosine[:, None, :], sine_table[:, None, :]))
    positions = jnp.arange(LEN, dtype=jnp.int32)
    q_rows = min(512, LEN)
    q_blocks = LEN // q_rows
    query_blocks = queries.reshape(q_blocks, q_rows, KV, groups, HD)
    pos_blocks = positions.reshape(q_blocks, q_rows)
    seg_blocks = segments.reshape(q_blocks, q_rows)

    def attend(pieces):
        query_block, query_pos, query_seg = pieces
        scores = low_back(jnp.einsum('qkgd,lkd->kqgl', query_block, key_rows, precision=highest) * score_scale)
        allowed = (positions[None, :] <= query_pos[:, None]) & (segments[None, :] == query_seg[:, None])
        scores = jnp.where(allowed[None, :, None, :], scores, neg_big)
        row_top = lax.optimization_barrier(jnp.max(scores, axis=-1, keepdims=True))
        exp_terms = jnp.exp(scores - row_top)
        probs = exp_terms / lax.optimization_barrier(jnp.sum(exp_terms, axis=-1, keepdims=True))
        return jnp.einsum('kqgl,lkd->qkgd', low(probs), values, precision=highest)
    attended = lax.map(jax.checkpoint(attend), (query_blocks, pos_blocks, seg_blocks))
    attended = low(low_back(attended.reshape(LEN, H * HD)))
    middle = tokens + low_back(jnp.dot(attended, o_weight, precision=highest))
    hidden = low(middle * rms_scale(middle) * ffn_gain)
    logits = low_back(jnp.dot(hidden, router_weight, precision=highest))
    expert_ids = jnp.arange(EXPERTS, dtype=jnp.int32)
    route_hit = routes[:, :, None] == expert_ids[None, None, :]
    chosen = lax.optimization_barrier(jnp.sum(jnp.where(route_hit, logits[:, None, :], 0.0), axis=-1))
    gate_weights = jax.nn.softmax(chosen, axis=-1)
    pair_hit = route_hit.reshape(N_CTX, BLOCK * TOPK, EXPERTS).astype(jnp.int32)
    earlier = jnp.cumsum(pair_hit, axis=1) - pair_hit
    slot_index = lax.optimization_barrier(jnp.sum(earlier * pair_hit, axis=-1))
    kept_pair = slot_index < CAP
    block_ids = jnp.arange(N_CTX, dtype=jnp.int32)[:, None]
    expert_of = routes.reshape(N_CTX, BLOCK * TOPK)
    target_row = jnp.where(kept_pair, (expert_of * N_CTX + block_ids) * CAP + slot_index, EXPERTS * N_CTX * CAP).reshape(-1)
    pair_token = jnp.arange(LEN * TOPK, dtype=jnp.int32) // TOPK
    slot_source = jnp.full((EXPERTS * N_CTX * CAP,), LEN, jnp.int32).at[target_row].set(pair_token, mode='drop')
    padded_hidden = jnp.concatenate([hidden, jnp.zeros((1, D), hidden.dtype)], axis=0)
    expert_in = low_back(padded_hidden[slot_source]).reshape(EXPERTS, N_CTX * CAP, D)
    gate_up = low_back(jnp.einsum('erd,edf->erf', expert_in, gate_up_weight, precision=highest))
    activated = low(jax.nn.silu(gate_up[..., :FF]) * gate_up[..., FF:])
    expert_out = low(low_back(jnp.einsum('erf,efd->erd', activated, down_weight, precision=highest)))
    padded_out = jnp.concatenate([expert_out.reshape(EXPERTS * N_CTX * CAP, D), jnp.zeros((1, D), expert_out.dtype)], axis=0)
    pair_out = padded_out[target_row].reshape(LEN, TOPK, D)
    pair_weight = gate_weights * kept_pair.reshape(LEN, TOPK).astype(gate_weights.dtype)
    return middle + lax.optimization_barrier(jnp.sum(pair_weight[:, :, None] * pair_out, axis=1))

def reference(tokens, segment_ids, routes, cotangent, q_weight, k_weight, v_weight, o_weight, router_weight, norm_gains, gate_up_weight, down_weight):
    params = (q_weight.astype(jnp.float32), k_weight.astype(jnp.float32), v_weight.astype(jnp.float32), o_weight.astype(jnp.float32), router_weight.astype(jnp.float32), norm_gains.astype(jnp.float32), gate_up_weight.astype(jnp.float32), down_weight.astype(jnp.float32))
    cosine, sine_table = rope_tables(jnp.arange(LEN, dtype=jnp.int32))

    def per_sequence(gradients, pieces):
        seq_tokens, seq_segments, seq_routes, seq_cotangent = pieces

        def closure(inputs, weights):
            return layer(inputs, weights, seq_segments, seq_routes, cosine, sine_table)
        result, pullback = jax.vjp(closure, seq_tokens.astype(jnp.float32), params)
        input_grad, weight_grads = pullback(seq_cotangent.astype(jnp.float32))
        gradients = tuple((running + addend for running, addend in zip(gradients, weight_grads)))
        return (gradients, (result.astype(jnp.bfloat16), input_grad.astype(jnp.bfloat16)))
    zero_grads = tuple((jnp.zeros_like(weight) for weight in params))
    gradients, (outputs, input_grads) = lax.scan(per_sequence, zero_grads, (tokens, segment_ids, routes, cotangent))
    return (outputs, input_grads, gradients[0], gradients[1], gradients[2], gradients[3], gradients[4], gradients[5], gradients[6], gradients[7])
```

```python
import jax
import jax.numpy as jnp
from jax import lax
from jax.sharding import Mesh, PartitionSpec as P

H = 32
KV = 4
HD = 128
TOPK = 8

eps_norm = 1e-06
rope_base = 1000000.0
neg_big = -1e30
f32 = jnp.float32
bf16 = jnp.bfloat16


def rms_scale(operand):
    return lax.rsqrt(jnp.mean(operand * operand, axis=-1, keepdims=True) + eps_norm)


def norm_back(operand, scale_rows, gain_vec, upstream):
    weighted = gain_vec * upstream
    inner_mean = jnp.mean(operand * weighted, axis=-1, keepdims=True)
    return scale_rows * weighted - operand * scale_rows * scale_rows * scale_rows * inner_mean


def rope_tables(positions, head_size):
    frequency = rope_base ** (-(jnp.arange(head_size // 2, dtype=f32) * 2.0 / head_size))
    angles = positions.astype(f32)[:, None] * frequency[None, :]
    angles = jnp.concatenate([angles, angles], axis=-1)
    return (jnp.cos(angles), jnp.sin(angles))


def rotate(operand, cosine, sine_table):
    half_width = operand.shape[-1] // 2
    turned = jnp.concatenate([-operand[..., half_width:], operand[..., :half_width]], axis=-1)
    return operand * cosine + turned * sine_table


def rotate_back(upstream, cosine, sine_table):
    shifted = upstream * sine_table
    half_width = upstream.shape[-1] // 2
    return upstream * cosine + jnp.concatenate(
        [shifted[..., half_width:], -shifted[..., :half_width]], axis=-1
    )


def dot(a, b):
    return jnp.dot(a, b, preferred_element_type=f32)


def dot_nt(a, b):
    return lax.dot_general(a, b, (((1,), (1,)), ((), ())), preferred_element_type=f32)


def dot_tn(a, b):
    return lax.dot_general(a, b, (((0,), (0,)), ((), ())), preferred_element_type=f32)


def take(v, index, axis=0):
    return lax.dynamic_index_in_dim(v, index, axis, keepdims=False)


def add_low(a, b):
    return (a.astype(f32) + b.astype(f32)).astype(bf16)


def flip(v, axis, bit):
    n = lax.axis_size(axis)
    return lax.ppermute(v, axis, [(i, i ^ bit) for i in range(n)])


def px(v):
    return flip(v, "cl", 1)


def py(v):
    return flip(v, "cl", 2)


def shift(v, by):
    n = lax.axis_size("sq")
    return lax.ppermute(v, "sq", [(i, (i + by) % n) for i in range(n)])


def bits_of(axis):
    n, bit, out = lax.axis_size(axis), 1, []
    while bit < n:
        out.append(bit)
        bit *= 2
    return out


def tree_gather(v, axes):
    v = v[None]
    for axis in reversed(axes):
        index = lax.axis_index(axis)
        for bit in bits_of(axis):
            other = flip(v, axis, bit)
            upper = (index & bit) != 0
            v = jnp.concatenate(
                [jnp.where(upper, other, v), jnp.where(upper, v, other)], axis=0
            )
    return v


def tree_scatter(v, axes):
    for axis in axes:
        index = lax.axis_index(axis)
        for bit in reversed(bits_of(axis)):
            half = v.shape[0] // 2
            upper = (index & bit) != 0
            own = jnp.where(upper, v[half:], v[:half])
            other = jnp.where(upper, v[:half], v[half:])
            v = own + flip(other, axis, bit)
    return v[0]


def dp_gather(v):
    v = v[None]
    index = lax.axis_index("dp")
    for bit in bits_of("dp"):
        other = flip(v, "dp", bit)
        upper = (index & bit) != 0
        v = jnp.concatenate([jnp.where(upper, other, v), jnp.where(upper, v, other)], axis=0)
    return v


def dp_scatter(v):
    index = lax.axis_index("dp")
    for bit in reversed(bits_of("dp")):
        half = v.shape[0] // 2
        upper = (index & bit) != 0
        own = lax.dynamic_slice_in_dim(v, jnp.where(upper, half, 0), half, 0)
        other = lax.dynamic_slice_in_dim(v, jnp.where(upper, 0, half), half, 0)
        v = own.astype(f32) + flip(other.astype(bf16), "dp", bit).astype(f32)
    return v[0]


def dp_sum(v):
    for bit in bits_of("dp"):
        v = v + flip(v.astype(bf16), "dp", bit).astype(f32)
    return v


def to_sequence(v):
    nl, n_dp, n_sq = v.shape[0], lax.axis_size("dp"), lax.axis_size("sq")
    zi = lax.axis_index("sq")
    got = []
    for m in range(nl):
        pairs = [
            (d * n_sq + z, (z // nl) * n_sq + nl * d + (m + z) % nl)
            for d in range(n_dp)
            for z in range(n_sq)
        ]
        got.append(lax.ppermute(take(v, (m + zi) % nl), ("dp", "sq"), pairs))
    return jnp.stack(got)


def from_sequence(v):
    nl, n_dp, n_sq = v.shape[0], lax.axis_size("dp"), lax.axis_size("sq")
    zi = lax.axis_index("sq")
    got = []
    for m in range(nl):
        pairs = [
            ((z // nl) * n_sq + nl * d + (m + z) % nl, d * n_sq + z)
            for d in range(n_dp)
            for z in range(n_sq)
        ]
        got.append(lax.ppermute(v[m], ("dp", "sq"), pairs))
    got = jnp.stack(got)
    return jnp.stack([take(got, (j - zi) % nl) for j in range(nl)])


def plane_gather(v):
    cl = lax.axis_index("cl")
    half = v.shape[1] // 2
    a, b = v[:, :half], v[:, half:]
    a1, b1 = px(a), py(b)
    a2, b2 = py(jnp.stack([a, a1])), px(jnp.stack([b, b1]))
    parts = [
        jnp.concatenate([a, b], axis=1),
        jnp.concatenate([a1, b2[0]], axis=1),
        jnp.concatenate([a2[0], b1], axis=1),
        jnp.concatenate([a2[1], b2[1]], axis=1),
    ]
    full = jnp.zeros((4,) + v.shape, v.dtype)
    for k in range(4):
        full = lax.dynamic_update_index_in_dim(full, parts[k], cl ^ k, 0)
    return dp_gather(full)


def plane_scatter(v):
    cl = lax.axis_index("cl")
    v = dp_scatter(v)
    half = v.shape[-1] // 2
    piece = lambda k, lo: take(v[:, :, lo : lo + half], cl ^ k)
    a = [piece(k, 0) for k in range(4)]
    b = [piece(k, half) for k in range(4)]
    ra = py(jnp.stack([a[2], a[3]]).astype(bf16))
    rb = px(jnp.stack([b[1], b[3]]).astype(bf16))
    a0, a1 = a[0] + ra[0].astype(f32), a[1] + ra[1].astype(f32)
    b0, b2 = b[0] + rb[0].astype(f32), b[2] + rb[1].astype(f32)
    a0 = a0 + px(a1.astype(bf16)).astype(f32)
    b0 = b0 + py(b2.astype(bf16)).astype(f32)
    return jnp.concatenate([a0, b0], axis=1)


def ring_gather(v):
    got = [v]
    for _ in range(lax.axis_size("sq") - 1):
        got.append(shift(got[-1], 1))
    return got


def ring_scatter(parts, low=True):
    moving = parts[-1]
    for t in range(len(parts) - 2, -1, -1):
        got = shift(moving.astype(bf16), -1)
        total = parts[t].astype(f32) + got.astype(f32)
        moving = total.astype(bf16) if (t or low) else total
    return moving


def column_cuts(width):
    units = width // 128
    first = max(1, (units * 5) // 16)
    last = max(0, (units - 2 * first) // 2)
    return [0, first * 128, 2 * first * 128, (2 * first + last) * 128, width]


def wide_gather(v):
    cuts = column_cuts(v.shape[1])
    ab, e, f = v[:, : cuts[2]], v[:, cuts[2] : cuts[3]], v[:, cuts[3] :]
    e1, f1 = px(e), py(f)
    z = ring_gather(ab)
    n = len(z)
    e2, f2 = py(jnp.stack([e, e1])), px(jnp.stack([f, f1]))
    e4 = jnp.stack([e, e1, e2[0], e2[1]])
    f4 = jnp.stack([f, f2[0], f1, f2[1]])
    ef = jnp.concatenate([e4, f4], axis=-1)
    a = jnp.stack([q[:, : cuts[1]] for q in z])
    b = jnp.stack([q[:, cuts[1] :] for q in z])
    a1, b1 = px(a), py(b)
    zef = ring_gather(ef)
    a2, b2 = py(jnp.stack([a, a1])), px(jnp.stack([b, b1]))
    a4 = jnp.stack([a, a1, a2[0], a2[1]], axis=1)
    b4 = jnp.stack([b, b2[0], b1, b2[1]], axis=1)
    return jnp.concatenate([a4, b4, jnp.stack(zef)], axis=-1)


def wide_scatter(v):
    cuts = column_cuts(v.shape[-1])
    a, b = v[..., : cuts[1]], v[..., cuts[1] : cuts[2]]
    ef = v[..., cuts[2] :]
    we = cuts[3] - cuts[2]
    ra = py(a[:, 2:])
    rb = px(jnp.stack([b[:, 1], b[:, 3]], axis=1))
    ef = ring_scatter([ef[t] for t in range(v.shape[0])])
    a = add_low(a[:, :2], ra)
    b = add_low(jnp.stack([b[:, 0], b[:, 2]], axis=1), rb)
    a = add_low(a[:, 0], px(a[:, 1]))
    b = add_low(b[:, 0], py(b[:, 1]))
    ab = jnp.concatenate([a, b], axis=-1)
    e, f = ef[..., :we], ef[..., we:]
    re = py(e[2:])
    rf = px(jnp.stack([f[1], f[3]]))
    e = add_low(e[:2], re)
    f = add_low(jnp.stack([f[0], f[2]]), rf)
    e = add_low(e[0], px(e[1]))
    f = add_low(f[0], py(f[1]))
    ab = ring_scatter([ab[t] for t in range(v.shape[0])])
    return jnp.concatenate([ab, e, f], axis=-1)


def on_device(
    tokens,
    segment_ids,
    routes,
    cotangent,
    q_weight,
    k_weight,
    v_weight,
    o_weight,
    router_weight,
    norm_gains,
    gate_up_weight,
    down_weight,
):
    n_dp, n_sq, n_cl = lax.axis_size("dp"), lax.axis_size("sq"), lax.axis_size("cl")
    dp, zi, cl = lax.axis_index("dp"), lax.axis_index("sq"), lax.axis_index("cl")
    nl, bl, width = tokens.shape
    rows = nl * bl
    n_ctx = n_sq * n_cl
    length = bl * n_ctx
    n_all = n_dp * n_ctx
    tp = n_cl * n_dp
    experts = n_ctx
    expert = zi * n_cl + cl
    capacity = max(2, (5 * bl * TOPK + 4 * experts - 1) // (4 * experts))
    ff = down_weight.shape[1]
    heads = H // tp
    hw = heads * HD
    kvw = 2 * HD // n_dp
    pack = hw + kvw
    score_scale = HD ** (-0.5)
    shard = width // n_all

    hit = jnp.any(
        routes[:, :, :, None] == jnp.arange(experts, dtype=jnp.int32), axis=2
    ).astype(bf16)
    below = jnp.tril(jnp.ones((bl, bl), bf16), -1)
    earlier = jnp.einsum("pq,jqe->jpe", below, hit, preferred_element_type=f32)
    codes = jnp.where(hit > 0, jnp.minimum(earlier + 1.0, capacity + 1.0), 0.0).astype(bf16)
    codes = jnp.pad(codes, ((0, 0), (0, 0), (0, 128 - experts)))

    small = jnp.concatenate(
        [router_weight.T.reshape(-1), norm_gains.reshape(-1)]
    )
    n_small = small.shape[0]
    n_router = experts * shard
    small = jnp.pad(small, (0, -n_small % 128)).reshape(-1, 128)
    small = tree_gather(small, ("dp", "sq", "cl")).reshape(n_all, -1)
    router_t = small[:, :n_router].reshape(n_all, experts, shard)
    router_t = jnp.transpose(router_t, (1, 0, 2)).reshape(experts, width)
    gains = small[:, n_router:n_small].reshape(-1).astype(f32)
    attn_gain = gains[:width]
    ffn_gain = gains[width : 2 * width]
    q_gain = gains[2 * width : 2 * width + HD]
    k_gain = gains[2 * width + HD :]

    inputs = to_sequence(tokens).reshape(rows, width).astype(f32)

    kv_weight = jnp.concatenate(
        [k_weight.reshape(shard, n_cl, HD), v_weight.reshape(shard, n_cl, HD)], axis=-1
    )
    packed = jnp.concatenate(
        [
            q_weight.reshape(shard, n_cl, n_dp, hw),
            kv_weight.reshape(shard, n_cl, n_dp, kvw),
        ],
        axis=-1,
    )
    packed = jnp.transpose(packed, (1, 2, 0, 3)).reshape(tp, shard, pack)
    packed = lax.all_to_all(packed, ("cl", "dp"), split_axis=0, concat_axis=0, tiled=True)
    packed = jnp.transpose(packed.reshape(n_cl, n_dp, shard, pack), (1, 0, 2, 3))
    qkv_w = jnp.zeros((n_dp, n_sq, n_cl, shard, pack), bf16)
    for t, piece in enumerate(ring_gather(packed)):
        qkv_w = lax.dynamic_update_index_in_dim(qkv_w, piece, (zi - t) % n_sq, 1)
    qkv_w = qkv_w.reshape(width, pack)

    o_pairs = []
    for f in range(n_all):
        r, q = f // n_sq, f % n_sq
        o_pairs.append((f, ((r % n_dp) * n_sq + q) * n_cl + r // n_dp))
    o_mine = lax.ppermute(o_weight, ("dp", "sq", "cl"), o_pairs)
    o_full = jnp.zeros((n_sq,) + o_mine.shape, bf16)
    for t, piece in enumerate(ring_gather(o_mine)):
        o_full = lax.dynamic_update_index_in_dim(o_full, piece, (zi - t) % n_sq, 0)
    o_full = o_full.reshape(hw, width)

    gu_full = dp_gather(gate_up_weight[0]).reshape(width, 2 * ff)
    down_full = jnp.concatenate(list(dp_gather(down_weight[0])), axis=1)

    upstream_low = to_sequence(jnp.concatenate([cotangent, codes], axis=-1)).reshape(rows, -1)
    upstream = upstream_low[:, :width].astype(f32)
    own_codes = upstream_low[:, width : width + experts].astype(f32)
    grads_all = wide_gather(upstream_low).reshape(n_ctx * rows, -1)

    block_of = (zi - jnp.arange(nl)) % nl
    d_ids = jnp.arange(n_dp)[:, None, None, None]
    c_ids = jnp.arange(n_cl)[None, :, None, None]
    positions = ((d_ids * nl + block_of[None, None, :, None]) * n_cl + c_ids) * bl + jnp.arange(
        bl
    )[None, None, None, :]
    positions = positions.reshape(length).astype(jnp.int32)
    segments = take(tree_gather(segment_ids, ("dp",)).reshape(n_dp * nl, length), zi)
    segments = segments.reshape(n_dp, nl, n_cl, bl)
    segments = jnp.stack([take(segments, (zi - m) % nl, 1) for m in range(nl)], axis=2)
    segments = segments.reshape(length)
    cosine, sine_table = rope_tables(positions, HD)
    cosine, sine_table = cosine[:, None, :], sine_table[:, None, :]

    first_scale = rms_scale(inputs)
    normed = (inputs * first_scale * attn_gain).astype(bf16)
    normed_all = plane_gather(normed).reshape(length, width)
    proj = dot(normed_all, qkv_w)
    q_proj = proj[:, :hw].reshape(length, heads, HD)
    kv_proj = dp_gather(proj[:, hw:])
    kv_proj = jnp.concatenate(list(kv_proj), axis=-1)
    k_proj = kv_proj[:, None, :HD]
    values = kv_proj[:, HD:].astype(bf16)
    q_scale = rms_scale(q_proj)
    k_scale = rms_scale(k_proj)
    queries = rotate(q_proj * q_scale * q_gain, cosine, sine_table).astype(bf16)
    keys = rotate(k_proj * k_scale * k_gain, cosine, sine_table).astype(bf16)[:, 0]
    allowed = (positions[None, :] <= positions[:, None]) & (
        segments[None, :] == segments[:, None]
    )
    scores = jnp.einsum("qhd,kd->hqk", queries, keys, preferred_element_type=f32) * score_scale
    scores = jnp.where(allowed[None], scores, neg_big)
    terms = jnp.exp(scores - jnp.max(scores, axis=-1, keepdims=True))
    probs = terms / jnp.sum(terms, axis=-1, keepdims=True)
    prob_low = probs.astype(bf16)
    attended = jnp.einsum("hqk,kd->qhd", prob_low, values, preferred_element_type=f32)
    attended = attended.reshape(length, hw).astype(bf16)
    mixed = plane_scatter(dot(attended, o_full).reshape(n_dp, n_cl, rows, width))
    middle = inputs + mixed
    second_scale = rms_scale(middle)
    hidden = (middle * second_scale * ffn_gain).astype(bf16)
    logits = dot_nt(hidden, router_t)
    routed = own_codes > 0
    top = jnp.max(jnp.where(routed, logits, neg_big), axis=-1, keepdims=True)
    gate_terms = jnp.where(routed, jnp.exp(logits - top), 0.0)
    gates = gate_terms / jnp.sum(gate_terms, axis=-1, keepdims=True)
    gates_high = gates.astype(bf16)
    gates_low = (gates - gates_high.astype(f32)).astype(bf16)
    extra = jnp.pad(
        jnp.concatenate([gates_high, gates_low], axis=-1), ((0, 0), (0, 128 - 2 * experts))
    )
    hidden_all = wide_gather(jnp.concatenate([hidden, extra], axis=-1)).reshape(n_ctx * rows, -1)

    n_rows = n_ctx * rows
    per = min(4, n_rows // bl)
    n_groups = n_rows // (per * bl)
    lanes = jnp.arange(128)
    code = jnp.sum(jnp.where(lanes == expert, grads_all[:, width:].astype(f32), 0.0), axis=-1)
    pick = (lanes == expert) | (lanes == experts + expert)
    gate_mine = jnp.sum(jnp.where(pick, hidden_all[:, width:].astype(f32), 0.0), axis=-1)
    in_group = (jnp.arange(n_rows) // bl) % per
    code = jnp.where((code > 0) & (code <= capacity), code + in_group * 128.0, -1.0)
    code = code.reshape(n_groups, 1, per * bl)
    slot_ids = jnp.arange(per * capacity)
    slot_ids = ((slot_ids // capacity) * 128 + slot_ids % capacity + 1).astype(f32)
    select = code == slot_ids[None, :, None]
    select_low = select.astype(bf16)
    n_slots = n_groups * per * capacity

    def pull(v):
        v = v.reshape(n_groups, per * bl, -1)
        got = jnp.einsum("grt,gtd->grd", select_low, v, preferred_element_type=f32)
        return got.astype(bf16).reshape(n_slots, -1)

    def push(v):
        v = v.reshape(n_groups, per * capacity, -1)
        got = jnp.einsum("grt,grd->gtd", select_low, v, preferred_element_type=f32)
        return got.astype(bf16).reshape(n_rows, -1)

    gate_slot = jnp.sum(
        jnp.where(select, gate_mine.reshape(n_groups, 1, per * bl), 0.0), axis=-1
    ).reshape(n_slots, 1)
    expert_in = pull(hidden_all[:, :width])
    grad_slot = pull(grads_all[:, :width]).astype(f32)
    gate_up = dot(expert_in, gu_full)
    gate_part, up_part = gate_up[:, :ff], gate_up[:, ff:]
    sigmoid_gate = jax.nn.sigmoid(gate_part)
    activated = (gate_part * sigmoid_gate * up_part).astype(bf16)
    expert_out = dot(activated, down_full).astype(bf16)
    out_wide = expert_out.astype(f32)
    pair_grad = jnp.sum(grad_slot * out_wide, axis=-1)
    moe = wide_scatter(push((gate_slot * out_wide).astype(bf16)).reshape(n_sq, n_cl, rows, width))
    output = (middle + moe.astype(f32)).astype(bf16)

    out_grad = (gate_slot * grad_slot).astype(bf16)
    act_grad = dot_nt(out_grad, down_full)
    gate_back = act_grad * up_part * sigmoid_gate * (1.0 + gate_part * (1.0 - sigmoid_gate))
    up_back = act_grad * gate_part * sigmoid_gate
    gu_grad = jnp.concatenate([gate_back, up_back], axis=-1).astype(bf16)
    row_grad = dot_nt(gu_grad, gu_full).astype(bf16)
    pair_token = jnp.sum(
        jnp.where(select, pair_grad.reshape(n_groups, per * capacity, 1), 0.0), axis=1
    ).reshape(n_rows, 1)
    pair_high = pair_token.astype(bf16)
    pair_low = (pair_token - pair_high.astype(f32)).astype(bf16)
    pair_extra = jnp.where(
        lanes == expert, pair_high, jnp.where(lanes == experts + expert, pair_low, 0)
    ).astype(bf16)
    back = wide_scatter(
        jnp.concatenate([push(row_grad), pair_extra], axis=-1).reshape(n_sq, n_cl, rows, -1)
    ).astype(f32)

    gu_share = dp_scatter(dot_tn(expert_in, gu_grad).reshape(n_dp, -1, 2 * ff))
    down_share = dp_scatter(
        jnp.stack(jnp.split(dot_tn(activated, out_grad), n_dp, axis=1))
    )

    pair_own = back[:, width : width + experts] + back[:, width + experts : width + 2 * experts]
    chosen_grad = gates * (pair_own - jnp.sum(gates * pair_own, axis=-1, keepdims=True))
    logit_grad = chosen_grad.astype(bf16)
    hidden_grad = back[:, :width] + dot(logit_grad, router_t)
    router_grad = dot_tn(logit_grad, hidden)
    ffn_gain_grad = jnp.sum(hidden_grad * middle * second_scale, axis=0)
    middle_grad = upstream + norm_back(middle, second_scale, ffn_gain, hidden_grad)

    middle_low = plane_gather(middle_grad.astype(bf16)).reshape(length, width)
    attended_grad = dot_nt(middle_low, o_full).astype(bf16).reshape(length, heads, HD)
    o_grad = dot_tn(attended, middle_low).reshape(n_sq, -1, width)
    o_share = ring_scatter([take(o_grad, (zi - t) % n_sq) for t in range(n_sq)])
    o_share = lax.ppermute(
        o_share, ("dp", "sq", "cl"), [(b, a) for a, b in o_pairs]
    ).astype(f32)
    prob_grad = jnp.einsum("qhd,kd->hqk", attended_grad, values, preferred_element_type=f32)
    inner_sum = jnp.sum(probs * prob_grad, axis=-1, keepdims=True)
    score_grad = (probs * (prob_grad - inner_sum)).astype(bf16)
    value_part = jnp.einsum("hqk,qhd->kd", prob_low, attended_grad, preferred_element_type=f32)
    key_part = (
        jnp.einsum("hqk,qhd->kd", score_grad, queries, preferred_element_type=f32) * score_scale
    )
    query_grad = (
        jnp.einsum("hqk,kd->qhd", score_grad, keys, preferred_element_type=f32) * score_scale
    )
    kv_sum = dp_sum(jnp.concatenate([key_part, value_part], axis=-1))
    key_rot_grad = rotate_back(kv_sum[:, None, :HD], cosine, sine_table)
    k_gain_grad = jnp.sum(key_rot_grad * k_proj * k_scale, axis=(0, 1))
    k_gain_grad = jnp.where(dp == 0, k_gain_grad, 0.0)
    k_low = norm_back(k_proj, k_scale, k_gain, key_rot_grad)[:, 0].astype(bf16)
    kv_low = jnp.concatenate([k_low, kv_sum[:, HD:].astype(bf16)], axis=-1)
    kv_low = lax.dynamic_slice_in_dim(kv_low, dp * kvw, kvw, 1)
    query_rot_grad = rotate_back(query_grad, cosine, sine_table)
    q_gain_grad = jnp.sum(query_rot_grad * q_proj * q_scale, axis=(0, 1))
    q_low = norm_back(q_proj, q_scale, q_gain, query_rot_grad).reshape(length, hw).astype(bf16)
    qkv_low = jnp.concatenate([q_low, kv_low], axis=-1)
    normed_grad = plane_scatter(dot_nt(qkv_low, qkv_w).reshape(n_dp, n_cl, rows, width))
    attn_gain_grad = jnp.sum(normed_grad * inputs * first_scale, axis=0)
    input_grad = middle_grad + norm_back(inputs, first_scale, attn_gain, normed_grad)
    input_grad = from_sequence(input_grad.astype(bf16).reshape(nl, bl, width))
    output = from_sequence(output.reshape(nl, bl, width))

    w_grad = dot_tn(normed_all, qkv_low).reshape(n_dp, n_sq, n_cl, shard, pack)
    w_grad = ring_scatter([take(w_grad, (zi - t) % n_sq, 1) for t in range(n_sq)])
    w_grad = jnp.transpose(w_grad, (1, 0, 2, 3)).reshape(tp, shard, pack)
    w_grad = lax.all_to_all(w_grad, ("cl", "dp"), split_axis=0, concat_axis=0, tiled=True)
    w_grad = jnp.transpose(w_grad.reshape(n_cl, n_dp, shard, pack), (2, 0, 1, 3)).astype(f32)
    q_share = w_grad[..., :hw].reshape(shard, -1)
    kv_share = w_grad[..., hw:].reshape(shard, n_cl, 2 * HD)
    k_share = kv_share[..., :HD].reshape(shard, -1)
    v_share = kv_share[..., HD:].reshape(shard, -1)

    gain_grads = jnp.concatenate([attn_gain_grad, ffn_gain_grad, q_gain_grad, k_gain_grad])
    router_grad = jnp.transpose(router_grad.reshape(experts, n_all, shard), (1, 0, 2))
    small_grad = jnp.concatenate(
        [router_grad.reshape(n_all, n_router), gain_grads.reshape(n_all, -1)], axis=-1
    )
    small_grad = jnp.pad(small_grad, ((0, 0), (0, -n_small % 128))).reshape(n_all, -1, 128)
    small_grad = tree_scatter(small_grad, ("dp", "sq", "cl")).reshape(-1)
    router_share = small_grad[:n_router].reshape(experts, shard).T
    gains_share = small_grad[n_router:n_small]
    return (
        output,
        input_grad,
        q_share,
        k_share,
        v_share,
        o_share,
        router_share,
        gains_share,
        gu_share[None],
        down_share[None],
    )


def solution(mesh):
    n_dp, n_ctx = mesh.devices.shape
    n_cl = KV
    fine = Mesh(mesh.devices.reshape(n_dp, n_ctx // n_cl, n_cl), ("dp", "sq", "cl"))
    ctx = ("sq", "cl")
    every = ("dp", "sq", "cl")
    rows = P("dp", ctx, None)
    placed = (
        rows,
        P("dp", None),
        rows,
        rows,
        P(every, None),
        P(every, None),
        P(every, None),
        P(every, None),
        P(every, None),
        P(every),
        P(ctx, "dp", None),
        P(ctx, None, "dp"),
    )
    return jax.shard_map(
        on_device,
        mesh=fine,
        in_specs=placed,
        out_specs=(
            rows,
            rows,
            P(every, None),
            P(every, None),
            P(every, None),
            P(every, None),
            P(every, None),
            P(every),
            P(ctx, "dp", None),
            P(ctx, None, "dp"),
        ),
        check_vma=False,
    )
```

```python
import jax
import jax.numpy as jnp
from jax import lax
from jax.experimental import pallas as pl
from jax.experimental.pallas import tpu as pltpu
from jax.sharding import Mesh, PartitionSpec as P

H = 32
KV = 4
HD = 128
TOPK = 8

eps_norm = 1e-06
rope_base = 1000000.0
neg_big = -1e30
f32 = jnp.float32
bf16 = jnp.bfloat16


def tie(*v):
    return lax.optimization_barrier(v)


def rms_scale(operand):
    return lax.rsqrt(jnp.mean(operand * operand, axis=-1, keepdims=True) + eps_norm)


def norm_back(operand, scale_rows, gain_vec, upstream):
    weighted = gain_vec * upstream
    inner_mean = jnp.mean(operand * weighted, axis=-1, keepdims=True)
    return scale_rows * weighted - operand * scale_rows * scale_rows * scale_rows * inner_mean


def rope_tables(positions, head_size):
    frequency = rope_base ** (-(jnp.arange(head_size // 2, dtype=f32) * 2.0 / head_size))
    angles = positions.astype(f32)[:, None] * frequency[None, :]
    angles = jnp.concatenate([angles, angles], axis=-1)
    return (jnp.cos(angles), jnp.sin(angles))


def rotate(operand, cosine, sine_table):
    half_width = operand.shape[-1] // 2
    turned = jnp.concatenate([-operand[..., half_width:], operand[..., :half_width]], axis=-1)
    return operand * cosine + turned * sine_table


def rotate_back(upstream, cosine, sine_table):
    shifted = upstream * sine_table
    half_width = upstream.shape[-1] // 2
    return upstream * cosine + jnp.concatenate(
        [shifted[..., half_width:], -shifted[..., :half_width]], axis=-1
    )


def dot(a, b):
    return jnp.dot(a, b, preferred_element_type=f32)


def dot_nt(a, b):
    return lax.dot_general(a, b, (((1,), (1,)), ((), ())), preferred_element_type=f32)


def dot_tn(a, b):
    return lax.dot_general(a, b, (((0,), (0,)), ((), ())), preferred_element_type=f32)


def take(v, index, axis=0):
    return lax.dynamic_index_in_dim(v, index, axis, keepdims=False)


def flip(v, axis, bit):
    n = lax.axis_size(axis)
    return lax.ppermute(v, axis, [(i, i ^ bit) for i in range(n)])


def px(v):
    return flip(v, "cl", 1)


def py(v):
    return flip(v, "cl", 2)


def shift(v, by):
    n = lax.axis_size("sq")
    return lax.ppermute(v, "sq", [(i, (i + by) % n) for i in range(n)])


def bits_of(axis):
    n, bit, out = lax.axis_size(axis), 1, []
    while bit < n:
        out.append(bit)
        bit *= 2
    return out


def every_gather(v):
    n = lax.axis_size("dp") * lax.axis_size("sq") * lax.axis_size("cl")
    v = jnp.broadcast_to(v[None], (n,) + v.shape)
    return lax.all_to_all(v, ("dp", "sq", "cl"), split_axis=0, concat_axis=0, tiled=True)


def every_scatter(v):
    v = lax.all_to_all(v, ("dp", "sq", "cl"), split_axis=0, concat_axis=0, tiled=True)
    return jnp.sum(v, axis=0)


def xor_groups(v, bit):
    rest = v.shape[1:]
    v = v.reshape((-1, 2, bit) + rest)
    return jnp.concatenate([v[:, 1:], v[:, :1]], axis=1).reshape((-1,) + rest)


def dp_gather(v):
    v = v[None]
    index = lax.axis_index("dp")
    for bit in bits_of("dp"):
        other = flip(v, "dp", bit)
        upper = (index & bit) != 0
        v = jnp.concatenate([jnp.where(upper, other, v), jnp.where(upper, v, other)], axis=0)
    return v


def dp_columns(v):
    v = v[None]
    index = lax.axis_index("dp")
    for bit in bits_of("dp"):
        other = flip(v, "dp", bit)
        other = jnp.swapaxes(xor_groups(jnp.swapaxes(other, 0, 1), bit), 0, 1)
        upper = (index & bit) != 0
        v = jnp.concatenate([jnp.where(upper, other, v), jnp.where(upper, v, other)], axis=0)
    return v


def dp_rows(v):
    v = v[None]
    for bit in bits_of("dp"):
        v = jnp.concatenate([v, flip(v, "dp", bit)], axis=0)
    return v


def dp_fold(parts):
    for bit in reversed(bits_of("dp")):
        parts = [
            parts[m].astype(f32) + flip(parts[m + bit].astype(bf16), "dp", bit).astype(f32)
            for m in range(bit)
        ]
    return parts[0]


def dp_sum(v):
    for bit in bits_of("dp"):
        v = v + xor_groups(flip(v.astype(bf16), "dp", bit), bit).astype(f32)
    return v


def to_sequence(v):
    nl, n_dp, n_sq = v.shape[0], lax.axis_size("dp"), lax.axis_size("sq")
    zi = lax.axis_index("sq")
    got = []
    for m in range(nl):
        pairs = [
            (d * n_sq + z, (z // nl) * n_sq + nl * d + (m + z) % nl)
            for d in range(n_dp)
            for z in range(n_sq)
        ]
        got.append(lax.ppermute(take(v, (m + zi) % nl), ("dp", "sq"), pairs))
    return jnp.stack(got)


def from_sequence(v):
    nl, n_dp, n_sq = v.shape[0], lax.axis_size("dp"), lax.axis_size("sq")
    zi = lax.axis_index("sq")
    got = []
    for m in range(nl):
        pairs = [
            ((z // nl) * n_sq + nl * d + (m + z) % nl, d * n_sq + z)
            for d in range(n_dp)
            for z in range(n_sq)
        ]
        got.append(lax.ppermute(v[m], ("dp", "sq"), pairs))
    got = jnp.stack(got)
    return jnp.stack([take(got, (j - zi) % nl) for j in range(nl)])


def head_pairs():
    n_dp, n_sq, n_cl = lax.axis_size("dp"), lax.axis_size("sq"), lax.axis_size("cl")
    pairs = []
    for f in range(n_dp * n_sq * n_cl):
        r, q = f // n_sq, f % n_sq
        pairs.append((f, ((r % n_dp) * n_sq + (q + r) % n_sq) * n_cl + r // n_dp))
    return pairs


def spread(v):
    h = v.shape[0] // 2
    a, b = v[:h], v[h:]
    a1, b1 = px(a), py(b)
    a2, b2 = py(a), px(b)
    a3, b3 = py(a1), px(b1)
    return [a, a1, a2, a3, b, b1, b2, b3]


def fold_first(v):
    ra, rb = py(v[:, 0, 2:].astype(bf16)), px(v[:, 1, 2:].astype(bf16))
    return v[:, :, :2], ra, rb


def fold_last(first):
    v, ra, rb = first
    a = v[:, 0].astype(f32) + ra.astype(f32)
    b = v[:, 1].astype(f32) + rb.astype(f32)
    a0 = a[:, 0] + px(a[:, 1].astype(bf16)).astype(f32)
    b0 = b[:, 0] + py(b[:, 1].astype(bf16)).astype(f32)
    return jnp.stack([a0, b0], axis=1)


def fold(v):
    return fold_last(fold_first(v[None]))[0]


def ring_gather(v):
    got = [v]
    for _ in range(lax.axis_size("sq") - 1):
        got.append(shift(got[-1], 1))
    return got


def ring_scatter(parts):
    moving = parts[1]
    for t in list(range(2, len(parts))) + [0]:
        got = shift(moving.astype(bf16), 1)
        moving = parts[t].astype(f32) + got.astype(f32)
    return moving


def pull_kernel(chosen, *refs):
    *pieces, main, tail = refs
    groups, slots = chosen.shape[:2]
    n = len(pieces) // groups
    width = main.shape[-1]
    for g in range(groups):
        rows = jnp.concatenate([piece[...] for piece in pieces[g * n : (g + 1) * n]], axis=0)
        got = jnp.dot(chosen[g], rows, preferred_element_type=f32).astype(bf16)
        main[pl.ds(g * slots, slots), :] = got[:, :width]
        tail[pl.ds(g * slots, slots), :] = got[:, width:]


def pull_pieces(chosen, pieces, width):
    slots = chosen.shape[0] * chosen.shape[1]
    rest = pieces[0].shape[1] - width
    return pl.pallas_call(
        pull_kernel,
        out_shape=(
            jax.ShapeDtypeStruct((slots, width), bf16),
            jax.ShapeDtypeStruct((slots, rest), bf16),
        ),
        name="pull",
    )(chosen, *pieces)


def pull_blocks_kernel(index, chosen, *refs):
    *blocks, out = refs
    rows = jnp.concatenate([block[0] for block in blocks], axis=0)
    out[...] = jnp.dot(chosen[0], rows, preferred_element_type=f32).astype(bf16)


def pull_blocks(index, chosen, blocks, width):
    groups, slots, depth = chosen.shape
    n = index.shape[1]
    block = (1, depth // n, width)
    specs = [pl.BlockSpec((1, slots, depth), lambda g, at: (g, 0, 0))]
    for i in range(n):
        specs.append(pl.BlockSpec(block, lambda g, at, i=i: (at[g, i], 0, 0)))
    return pl.pallas_call(
        pull_blocks_kernel,
        grid_spec=pltpu.PrefetchScalarGridSpec(
            num_scalar_prefetch=1,
            grid=(groups,),
            in_specs=specs,
            out_specs=pl.BlockSpec((slots, width), lambda g, at: (g, 0)),
        ),
        out_shape=jax.ShapeDtypeStruct((groups * slots, width), bf16),
        name="pull_blocks",
    )(index, chosen, *([blocks] * n))


def on_device(
    tokens,
    segment_ids,
    routes,
    cotangent,
    q_weight,
    k_weight,
    v_weight,
    o_weight,
    router_weight,
    norm_gains,
    gate_up_weight,
    down_weight,
):
    n_dp, n_sq, n_cl = lax.axis_size("dp"), lax.axis_size("sq"), lax.axis_size("cl")
    dp, zi, cl = lax.axis_index("dp"), lax.axis_index("sq"), lax.axis_index("cl")
    nl, bl, width = tokens.shape
    rows = nl * bl
    n_ctx = n_sq * n_cl
    length = bl * n_ctx
    n_all = n_dp * n_ctx
    tp = n_cl * n_dp
    experts = n_ctx
    expert = zi * n_cl + cl
    capacity = max(2, (5 * bl * TOPK + 4 * experts - 1) // (4 * experts))
    ff = down_weight.shape[1]
    heads = H // tp
    hw = heads * HD
    kvw = 2 * HD // n_dp
    pack = hw + kvw
    score_scale = HD ** (-0.5)
    shard = width // n_all

    hit = jnp.any(
        routes[:, :, :, None] == jnp.arange(experts, dtype=jnp.int32), axis=2
    ).astype(bf16)
    below = jnp.tril(jnp.ones((bl, bl), bf16), -1)
    earlier = jnp.einsum("pq,jqe->jpe", below, hit, preferred_element_type=f32)
    codes = jnp.where(hit > 0, jnp.minimum(earlier + 1.0, capacity + 1.0), 0.0).astype(bf16)
    codes = jnp.pad(codes, ((0, 0), (0, 0), (0, 128 - experts)))

    small = jnp.concatenate(
        [router_weight.T.reshape(-1), norm_gains.reshape(-1)]
    )
    n_small = small.shape[0]
    n_router = experts * shard
    small = jnp.pad(small, (0, -n_small % 128)).reshape(-1, 128)
    small = every_gather(small).reshape(n_all, -1)
    router_t = small[:, :n_router].reshape(n_all, experts, shard)
    router_t = jnp.transpose(router_t, (1, 0, 2)).reshape(experts, width)
    gains = small[:, n_router:n_small].reshape(-1).astype(f32)
    attn_gain = gains[:width]
    ffn_gain = gains[width : 2 * width]
    q_gain = gains[2 * width : 2 * width + HD]
    k_gain = gains[2 * width + HD :]

    inputs_low = to_sequence(tokens).reshape(rows, width)
    inputs = inputs_low.astype(f32)
    inputs_all = dp_rows(jnp.concatenate(spread(inputs_low))).reshape(length, width).astype(f32)

    kv_weight = jnp.concatenate(
        [k_weight.reshape(shard, n_cl, HD), v_weight.reshape(shard, n_cl, HD)], axis=-1
    )
    packed = jnp.concatenate(
        [
            q_weight.reshape(shard, n_cl, n_dp, hw),
            kv_weight.reshape(shard, n_cl, n_dp, kvw),
        ],
        axis=-1,
    )
    packed = jnp.transpose(packed, (1, 2, 0, 3)).reshape(tp, shard, pack)
    packed = lax.all_to_all(packed, ("cl", "dp"), split_axis=0, concat_axis=0, tiled=True)
    packed = jnp.transpose(packed.reshape(n_cl, n_dp, shard, pack), (1, 0, 2, 3))
    qkv_w = jnp.zeros((n_dp, n_sq, n_cl, shard, pack), bf16)
    rank = cl * n_dp + dp
    o_mine = lax.ppermute(o_weight, ("dp", "sq", "cl"), head_pairs())
    qkv_pieces = [packed, shift(packed, 1)]
    qkv_pieces[1], o_mine = tie(qkv_pieces[1], o_mine)
    for _ in range(2, n_sq):
        qkv_pieces.append(shift(qkv_pieces[-1], 1))

    upstream_low = jnp.concatenate([cotangent, codes], axis=-1)
    qkv_pieces[-2], upstream_low = tie(qkv_pieces[-2], upstream_low)
    qkv_pieces[-1] = shift(qkv_pieces[-2], 1)
    upstream_low = to_sequence(upstream_low).reshape(rows, -1)
    upstream = upstream_low[:, :width].astype(f32)
    own_codes = upstream_low[:, width : width + experts].astype(f32)
    qkv_pieces[-1], upstream_low, o_mine = tie(qkv_pieces[-1], upstream_low, o_mine)
    grads_all = lax.all_gather(upstream_low, ("sq", "cl"))
    o_pieces = [o_mine, shift(o_mine, 1)]
    for t, piece in enumerate(qkv_pieces):
        qkv_w = lax.dynamic_update_index_in_dim(qkv_w, piece, (zi - t) % n_sq, 1)
    qkv_w = qkv_w.reshape(width, pack)

    gu_full = dp_gather(gate_up_weight[0]).reshape(width, 2 * ff)
    down_full = jnp.concatenate(list(dp_gather(down_weight[0])), axis=1)

    order = jnp.array([[0, 1, 2, 3], [0, 2, 1, 3]], jnp.int32)
    chip_of = order ^ cl
    hb = nl // 2
    block_of = (zi - jnp.arange(nl).reshape(2, hb)) % nl
    d_ids = (jnp.arange(n_dp) ^ dp)[:, None, None, None]
    block_ids = (d_ids * nl + block_of[None, :, None, :]) * n_cl + chip_of[None, :, :, None]
    positions = block_ids[..., None] * bl + jnp.arange(bl)
    positions = positions.reshape(length).astype(jnp.int32)
    segments = take(dp_gather(segment_ids).reshape(n_dp * nl, length), zi)
    segments = segments.reshape(1, n_dp * nl * n_cl, bl)
    found = block_ids.reshape(-1, 1, 1) == jnp.arange(n_dp * nl * n_cl)[None, :, None]
    segments = jnp.sum(jnp.where(found, segments, 0), axis=1).reshape(length)
    cosine, sine_table = rope_tables(positions, HD)
    cosine, sine_table = cosine[:, None, :], sine_table[:, None, :]

    first_scale = rms_scale(inputs)
    inputs_all, gu_full, down_full = tie(inputs_all, gu_full, down_full)
    normed_all = (inputs_all * rms_scale(inputs_all) * attn_gain).astype(bf16)
    proj = dot(normed_all, qkv_w)
    q_proj = proj[:, :hw].reshape(length, heads, HD)
    kv_proj = dp_columns(proj[:, hw:].reshape(n_dp, -1, kvw)).reshape(n_dp, length, kvw)
    kv_proj = jnp.concatenate(list(kv_proj), axis=-1)
    k_proj = kv_proj[:, None, :HD]
    values = kv_proj[:, HD:].astype(bf16)
    q_scale = rms_scale(q_proj)
    k_scale = rms_scale(k_proj)
    queries = rotate(q_proj * q_scale * q_gain, cosine, sine_table).astype(bf16)
    keys = rotate(k_proj * k_scale * k_gain, cosine, sine_table).astype(bf16)[:, 0]
    queries, o_pieces[1] = tie(queries, o_pieces[1])
    o_pieces.append(shift(o_pieces[1], 1))
    values, o_pieces[2] = tie(values, o_pieces[2])
    for _ in range(3, n_sq):
        o_pieces.append(shift(o_pieces[-1], 1))
    allowed = (positions[None, :] <= positions[:, None]) & (
        segments[None, :] == segments[:, None]
    )
    scores = jnp.einsum("qhd,kd->hqk", queries, keys, preferred_element_type=f32) * score_scale
    scores = jnp.where(allowed[None], scores, neg_big)
    terms = jnp.exp(scores - jnp.max(scores, axis=-1, keepdims=True))
    probs = terms / jnp.sum(terms, axis=-1, keepdims=True)
    prob_low = probs.astype(bf16)
    attended = jnp.einsum("hqk,kd->qhd", prob_low, values, preferred_element_type=f32)
    attended = attended.reshape(length, hw).astype(bf16)
    attended, o_pieces[-1] = tie(attended, o_pieces[-1])
    o_full = jnp.zeros((n_sq,) + o_weight.shape, bf16)
    for t, piece in enumerate(o_pieces):
        o_full = lax.dynamic_update_index_in_dim(o_full, piece, (zi - t - rank) % n_sq, 0)
    o_full = o_full.reshape(hw, width)
    mixed = [dot(attended_m, o_full) for attended_m in attended.reshape(n_dp, -1, hw)]
    mixed = fold(dp_fold(mixed).reshape(2, n_cl, rows // 2, width)).reshape(rows, width)
    middle = inputs + mixed
    second_scale = rms_scale(middle)
    hidden = (middle * second_scale * ffn_gain).astype(bf16)
    logits = dot_nt(hidden, router_t)
    routed = own_codes > 0
    top = jnp.max(jnp.where(routed, logits, neg_big), axis=-1, keepdims=True)
    gate_terms = jnp.where(routed, jnp.exp(logits - top), 0.0)
    gates = gate_terms / jnp.sum(gate_terms, axis=-1, keepdims=True)
    gates_high = gates.astype(bf16)
    gates_low = (gates - gates_high.astype(f32)).astype(bf16)
    extra = jnp.pad(
        jnp.concatenate([gates_high, gates_low], axis=-1), ((0, 0), (0, 128 - 2 * experts))
    )
    hidden_wide = jnp.concatenate([hidden, extra], axis=-1)

    lanes = jnp.arange(128)
    half = rows // 2
    n_slot = n_cl * hb * capacity
    z_of = (zi - jnp.arange(n_sq)) % n_sq
    at = (z_of[:, None, None] * n_cl + chip_of) * 2 + jnp.arange(2)[:, None]
    at = at.reshape(2 * n_sq, n_cl).astype(jnp.int32)
    code = jnp.where(lanes == expert, grads_all[:, :, width:].astype(f32), 0.0)
    code = jnp.sum(code, axis=-1).reshape(1, n_ctx * 2, half)
    found = at.reshape(-1, 1, 1) == jnp.arange(n_ctx * 2)[:, None]
    code = jnp.sum(jnp.where(found, code, 0.0), axis=1)
    code = jnp.where(code <= capacity, code, 0.0).reshape(n_sq, 2, 1, n_cl * half)
    place = (jnp.arange(n_cl * half) // bl) * 128.0
    ids = jnp.arange(n_slot)
    ids = ((ids // capacity) * 128 + ids % capacity + 1).astype(f32)
    select = (jnp.where(code > 0, code + place, -1.0) == ids[:, None]).astype(bf16)
    pick = (lanes == expert) | (lanes == experts + expert)

    def push(chosen, v):
        v = v.reshape(chosen.shape[:2] + (-1,))
        got = jnp.einsum("grt,grd->gtd", chosen, v, preferred_element_type=f32)
        return got.astype(bf16)

    per = 2
    n_chunk = n_sq // per
    select = select.reshape(n_chunk, per * 2, n_slot, -1)
    grad_slots = pull_blocks(
        at, select.reshape((-1,) + select.shape[2:]), grads_all.reshape(n_ctx * 2, half, -1), width
    )
    grad_slots = list(grad_slots.reshape(n_chunk, -1, width))

    ins, actives, out_grads, gu_grads, backs = [], [], [], [], []
    arrived = []
    moving = hidden_wide
    for t in range(n_sq):
        arrived += spread(moving)
        if t == 0:
            moving, grad_slots = tie(shift(moving, 1), grad_slots)
        elif t + 1 < n_sq:
            moving = shift(moving, 1)
    for chunk in range(n_chunk):
        pieces = arrived[chunk * per * 8 : (chunk + 1) * per * 8]
        chosen = select[chunk]
        expert_in, gate_lanes = pull_pieces(chosen, pieces, width)
        gate_slot = jnp.sum(
            jnp.where(pick, gate_lanes.astype(f32), 0.0), axis=-1, keepdims=True
        )
        grad_slot = grad_slots[chunk].astype(f32)
        gate_up = dot(expert_in, gu_full)
        gate_part, up_part = gate_up[:, :ff], gate_up[:, ff:]
        sigmoid_gate = jax.nn.sigmoid(gate_part)
        activated = (gate_part * sigmoid_gate * up_part).astype(bf16)
        if chunk:
            activated, back_first = tie(activated, back_first)
            backs += list(fold_last(back_first))
        expert_out = dot(activated, down_full).astype(bf16)
        out_wide = expert_out.astype(f32)
        pair_grad = jnp.sum(grad_slot * out_wide, axis=-1, keepdims=True)
        out_grad = (gate_slot * grad_slot).astype(bf16)
        act_grad = dot_nt(out_grad, down_full)
        gate_back = act_grad * up_part * sigmoid_gate * (1.0 + gate_part * (1.0 - sigmoid_gate))
        up_back = act_grad * gate_part * sigmoid_gate
        gu_grad = jnp.concatenate([gate_back, up_back], axis=-1).astype(bf16)
        if chunk:
            gu_grad, backs = tie(gu_grad, backs)
        row_grad = dot_nt(gu_grad, gu_full).astype(bf16)
        pair_high = pair_grad.astype(bf16)
        pair_low = (pair_grad - pair_high.astype(f32)).astype(bf16)
        pair_extra = jnp.where(
            lanes == expert, pair_high, jnp.where(lanes == experts + expert, pair_low, 0)
        ).astype(bf16)
        moe = (gate_slot * out_wide).astype(bf16)
        back = push(chosen, jnp.concatenate([row_grad, moe, pair_extra], axis=-1))
        back_first = fold_first(back.reshape(per, 2, n_cl, half, -1))
        ins.append(expert_in)
        actives.append(activated)
        out_grads.append(out_grad)
        gu_grads.append(gu_grad)
    backs = [v.reshape(rows, -1) for v in backs + list(fold_last(back_first))]
    back = ring_scatter(backs).astype(bf16).astype(f32)
    output = (middle + back[:, width : 2 * width]).astype(bf16)

    pair_own = back[:, 2 * width :]
    pair_own = pair_own[:, :experts] + pair_own[:, experts : 2 * experts]
    chosen_grad = gates * (pair_own - jnp.sum(gates * pair_own, axis=-1, keepdims=True))
    logit_grad = chosen_grad.astype(bf16)
    hidden_grad = back[:, :width] + dot(logit_grad, router_t)
    router_grad = dot_tn(logit_grad, hidden)
    ffn_gain_grad = jnp.sum(hidden_grad * middle * second_scale, axis=0)
    middle_grad = upstream + norm_back(middle, second_scale, ffn_gain, hidden_grad)

    middle_low = dp_rows(jnp.concatenate(spread(middle_grad.astype(bf16)))).reshape(length, width)
    o_grad = dot_tn(attended, middle_low).reshape(n_sq, -1, width)
    attended_grad = dot_nt(middle_low, o_full).astype(bf16).reshape(length, heads, HD)
    attended_grad, o_grad = tie(attended_grad, o_grad)
    o_parts = [take(o_grad, (zi - t - rank) % n_sq) for t in range(n_sq)]
    o_got = shift(o_parts[1].astype(bf16), 1)
    prob_grad = jnp.einsum("qhd,kd->hqk", attended_grad, values, preferred_element_type=f32)
    inner_sum = jnp.sum(probs * prob_grad, axis=-1, keepdims=True)
    score_grad = (probs * (prob_grad - inner_sum)).astype(bf16)
    value_part = jnp.einsum("hqk,qhd->kd", prob_low, attended_grad, preferred_element_type=f32)
    key_part = (
        jnp.einsum("hqk,qhd->kd", score_grad, queries, preferred_element_type=f32) * score_scale
    )
    query_grad = (
        jnp.einsum("hqk,kd->qhd", score_grad, keys, preferred_element_type=f32) * score_scale
    )
    kv_sum = jnp.concatenate([key_part, value_part], axis=-1).reshape(n_dp, -1, 2 * HD)
    kv_sum, o_got = tie(kv_sum, o_got)
    o_got = o_parts[2].astype(f32) + o_got.astype(f32)
    o_got = shift(o_got.astype(bf16), 1)
    kv_sum = dp_sum(kv_sum).reshape(length, 2 * HD)
    query_grad, o_got = tie(query_grad, o_got)
    for t in list(range(3, n_sq)) + [0]:
        o_got = o_parts[t].astype(f32) + o_got.astype(f32)
        if t:
            o_got = shift(o_got.astype(bf16), 1)
    o_share = lax.ppermute(
        o_got.astype(bf16), ("dp", "sq", "cl"), [(b, a) for a, b in head_pairs()]
    ).astype(f32)
    key_rot_grad = rotate_back(kv_sum[:, None, :HD], cosine, sine_table)
    k_gain_grad = jnp.sum(key_rot_grad * k_proj * k_scale, axis=(0, 1))
    k_gain_grad = jnp.where(dp == 0, k_gain_grad, 0.0)
    k_low = norm_back(k_proj, k_scale, k_gain, key_rot_grad)[:, 0].astype(bf16)
    kv_low = jnp.concatenate([k_low, kv_sum[:, HD:].astype(bf16)], axis=-1)
    kv_low = lax.dynamic_slice_in_dim(kv_low, dp * kvw, kvw, 1)
    query_rot_grad = rotate_back(query_grad, cosine, sine_table)
    q_gain_grad = jnp.sum(query_rot_grad * q_proj * q_scale, axis=(0, 1))
    q_low = norm_back(q_proj, q_scale, q_gain, query_rot_grad).reshape(length, hw).astype(bf16)
    qkv_low = jnp.concatenate([q_low, kv_low], axis=-1)
    qkv_low, gu_grads, out_grads = tie(qkv_low, gu_grads, out_grads)
    w_grad = dot_tn(normed_all, qkv_low).reshape(n_dp, n_sq, n_cl, shard, pack)
    w_parts = [take(w_grad, (zi - t) % n_sq, 1) for t in range(n_sq)]
    w_got = shift(w_parts[1].astype(bf16), 1)
    normed_grad = [dot_nt(low_m, qkv_w) for low_m in qkv_low.reshape(n_dp, -1, pack)]
    normed_first = fold_first(dp_fold(normed_grad).reshape(1, 2, n_cl, rows // 2, width))
    normed_first, w_got = tie(normed_first, w_got)
    w_got = shift((w_parts[2] + w_got.astype(f32)).astype(bf16), 1)
    normed_grad = fold_last(normed_first).reshape(rows, width)
    normed_grad, w_got = tie(normed_grad, w_got)
    for t in range(3, n_sq):
        w_got = shift((w_parts[t] + w_got.astype(f32)).astype(bf16), 1)
    attn_gain_grad = jnp.sum(normed_grad * inputs * first_scale, axis=0)
    input_grad = middle_grad + norm_back(inputs, first_scale, attn_gain, normed_grad)
    input_grad = from_sequence(input_grad.astype(bf16).reshape(nl, bl, width))
    output = from_sequence(output.reshape(nl, bl, width))

    gu_grad = jnp.concatenate(gu_grads)
    activated = jnp.concatenate(actives)

    def columns(parts, m):
        size = width // n_dp
        at = (dp ^ m) * size
        return jnp.concatenate([lax.dynamic_slice_in_dim(v, at, size, 1) for v in parts])

    gu_share = dp_fold([dot_tn(columns(ins, m), gu_grad) for m in range(n_dp)])
    down_share = dp_fold([dot_tn(activated, columns(out_grads, m)) for m in range(n_dp)])

    w_grad = (w_parts[0] + w_got.astype(f32)).astype(bf16)
    w_grad = jnp.transpose(w_grad, (1, 0, 2, 3)).reshape(tp, shard, pack)
    w_grad = lax.all_to_all(w_grad, ("cl", "dp"), split_axis=0, concat_axis=0, tiled=True)
    w_grad = jnp.transpose(w_grad.reshape(n_cl, n_dp, shard, pack), (2, 0, 1, 3)).astype(f32)
    q_share = w_grad[..., :hw].reshape(shard, -1)
    kv_share = w_grad[..., hw:].reshape(shard, n_cl, 2 * HD)
    k_share = kv_share[..., :HD].reshape(shard, -1)
    v_share = kv_share[..., HD:].reshape(shard, -1)

    gain_grads = jnp.concatenate([attn_gain_grad, ffn_gain_grad, q_gain_grad, k_gain_grad])
    router_grad = jnp.transpose(router_grad.reshape(experts, n_all, shard), (1, 0, 2))
    small_grad = jnp.concatenate(
        [router_grad.reshape(n_all, n_router), gain_grads.reshape(n_all, -1)], axis=-1
    )
    small_grad = jnp.pad(small_grad, ((0, 0), (0, -n_small % 128))).reshape(n_all, -1, 128)
    small_grad = every_scatter(small_grad).reshape(-1)
    router_share = small_grad[:n_router].reshape(experts, shard).T
    gains_share = small_grad[n_router:n_small]
    return (
        output,
        input_grad,
        q_share,
        k_share,
        v_share,
        o_share,
        router_share,
        gains_share,
        gu_share[None],
        down_share[None],
    )


def solution(mesh):
    n_dp, n_ctx = mesh.devices.shape
    n_cl = KV
    fine = Mesh(mesh.devices.reshape(n_dp, n_ctx // n_cl, n_cl), ("dp", "sq", "cl"))
    ctx = ("sq", "cl")
    every = ("dp", "sq", "cl")
    rows = P("dp", ctx, None)
    placed = (
        rows,
        P("dp", None),
        rows,
        rows,
        P(every, None),
        P(every, None),
        P(every, None),
        P(every, None),
        P(every, None),
        P(every),
        P(ctx, "dp", None),
        P(ctx, None, "dp"),
    )
    return jax.shard_map(
        on_device,
        mesh=fine,
        in_specs=placed,
        out_specs=(
            rows,
            rows,
            P(every, None),
            P(every, None),
            P(every, None),
            P(every, None),
            P(every, None),
            P(every),
            P(ctx, "dp", None),
            P(ctx, None, "dp"),
        ),
        check_vma=False,
    )
```

```python
import jax
import jax.numpy as jnp
from jax import lax
from jax.experimental import pallas as pl
from jax.sharding import Mesh, PartitionSpec as P

H = 32
KV = 4
HD = 128
TOPK = 8
BLOCK = 64

eps_norm = 1e-06
rope_base = 1000000.0
neg_big = -1e30
f32 = jnp.float32
bf16 = jnp.bfloat16


def tie(*v):
    return lax.optimization_barrier(v)


def rms_scale(operand):
    return lax.rsqrt(jnp.mean(operand * operand, axis=-1, keepdims=True) + eps_norm)


def norm_back(operand, scale_rows, gain_vec, upstream):
    weighted = gain_vec * upstream
    inner_mean = jnp.mean(operand * weighted, axis=-1, keepdims=True)
    return scale_rows * weighted - operand * scale_rows * scale_rows * scale_rows * inner_mean


def rope_tables(positions, head_size):
    frequency = rope_base ** (-(jnp.arange(head_size // 2, dtype=f32) * 2.0 / head_size))
    angles = positions.astype(f32)[:, None] * frequency[None, :]
    angles = jnp.concatenate([angles, angles], axis=-1)
    return (jnp.cos(angles), jnp.sin(angles))


def rotate(operand, cosine, sine_table):
    half_width = operand.shape[-1] // 2
    turned = jnp.concatenate([-operand[..., half_width:], operand[..., :half_width]], axis=-1)
    return operand * cosine + turned * sine_table


def rotate_back(upstream, cosine, sine_table):
    shifted = upstream * sine_table
    half_width = upstream.shape[-1] // 2
    return upstream * cosine + jnp.concatenate(
        [shifted[..., half_width:], -shifted[..., :half_width]], axis=-1
    )


def dot(a, b):
    return jnp.dot(a, b, preferred_element_type=f32)


def dot_nt(a, b):
    return lax.dot_general(a, b, (((1,), (1,)), ((), ())), preferred_element_type=f32)


def dot_tn(a, b):
    return lax.dot_general(a, b, (((0,), (0,)), ((), ())), preferred_element_type=f32)


def take(v, index, axis=0):
    return lax.dynamic_index_in_dim(v, index, axis, keepdims=False)


def flip(v, axis, bit):
    n = lax.axis_size(axis)
    return lax.ppermute(v, axis, [(i, i ^ bit) for i in range(n)])


def px(v):
    return flip(v, "cl", 1)


def py(v):
    return flip(v, "cl", 2)


def shift(v, by):
    n = lax.axis_size("sq")
    return lax.ppermute(v, "sq", [(i, (i + by) % n) for i in range(n)])


def bits_of(axis):
    n, bit, out = lax.axis_size(axis), 1, []
    while bit < n:
        out.append(bit)
        bit *= 2
    return out


def every_gather(v):
    n = lax.axis_size("dp") * lax.axis_size("sq") * lax.axis_size("cl")
    v = jnp.broadcast_to(v[None], (n,) + v.shape)
    return lax.all_to_all(v, ("dp", "sq", "cl"), split_axis=0, concat_axis=0, tiled=True)


def every_scatter(v):
    v = lax.all_to_all(v, ("dp", "sq", "cl"), split_axis=0, concat_axis=0, tiled=True)
    return jnp.sum(v, axis=0)


def xor_groups(v, bit):
    rest = v.shape[1:]
    v = v.reshape((-1, 2, bit) + rest)
    return jnp.concatenate([v[:, 1:], v[:, :1]], axis=1).reshape((-1,) + rest)


def dp_gather(v):
    v = v[None]
    index = lax.axis_index("dp")
    for bit in bits_of("dp"):
        other = flip(v, "dp", bit)
        upper = (index & bit) != 0
        v = jnp.concatenate([jnp.where(upper, other, v), jnp.where(upper, v, other)], axis=0)
    return v


def dp_columns(v):
    v = v[None]
    index = lax.axis_index("dp")
    for bit in bits_of("dp"):
        other = flip(v, "dp", bit)
        other = jnp.swapaxes(xor_groups(jnp.swapaxes(other, 0, 1), bit), 0, 1)
        upper = (index & bit) != 0
        v = jnp.concatenate([jnp.where(upper, other, v), jnp.where(upper, v, other)], axis=0)
    return v


def dp_rows(v):
    v = v[None]
    for bit in bits_of("dp"):
        v = jnp.concatenate([v, flip(v, "dp", bit)], axis=0)
    return v


def dp_fold(parts):
    for bit in reversed(bits_of("dp")):
        parts = [
            parts[m].astype(f32) + flip(parts[m + bit].astype(bf16), "dp", bit).astype(f32)
            for m in range(bit)
        ]
    return parts[0]


def dp_sum(v):
    for bit in bits_of("dp"):
        v = v + xor_groups(flip(v.astype(bf16), "dp", bit), bit).astype(f32)
    return v


def to_sequence(v):
    nl, n_dp, n_sq = v.shape[0], lax.axis_size("dp"), lax.axis_size("sq")
    zi = lax.axis_index("sq")
    got = []
    for m in range(nl):
        pairs = [
            (d * n_sq + z, (z // nl) * n_sq + nl * d + (m + z) % nl)
            for d in range(n_dp)
            for z in range(n_sq)
        ]
        got.append(lax.ppermute(take(v, (m + zi) % nl), ("dp", "sq"), pairs))
    return jnp.stack(got)


def from_sequence(v):
    nl, n_dp, n_sq = v.shape[0], lax.axis_size("dp"), lax.axis_size("sq")
    zi = lax.axis_index("sq")
    got = []
    for m in range(nl):
        pairs = [
            ((z // nl) * n_sq + nl * d + (m + z) % nl, d * n_sq + z)
            for d in range(n_dp)
            for z in range(n_sq)
        ]
        got.append(lax.ppermute(v[m], ("dp", "sq"), pairs))
    got = jnp.stack(got)
    return jnp.stack([take(got, (j - zi) % nl) for j in range(nl)])


def head_pairs():
    n_dp, n_sq, n_cl = lax.axis_size("dp"), lax.axis_size("sq"), lax.axis_size("cl")
    pairs = []
    for f in range(n_dp * n_sq * n_cl):
        r, q = f // n_sq, f % n_sq
        pairs.append((f, ((r % n_dp) * n_sq + (q + r) % n_sq) * n_cl + r // n_dp))
    return pairs


def spread(v):
    h = v.shape[0] // 2
    a, b = v[:h], v[h:]
    a1, b1 = px(a), py(b)
    a2, b2 = py(a), px(b)
    a3, b3 = py(a1), px(b1)
    return [a, a1, a2, a3, b, b1, b2, b3]


def fold_first(v):
    ra, rb = py(v[:, 0, 2:].astype(bf16)), px(v[:, 1, 2:].astype(bf16))
    return v[:, :, :2], ra, rb


def fold_last(first):
    v, ra, rb = first
    a = v[:, 0].astype(f32) + ra.astype(f32)
    b = v[:, 1].astype(f32) + rb.astype(f32)
    a0 = a[:, 0] + px(a[:, 1].astype(bf16)).astype(f32)
    b0 = b[:, 0] + py(b[:, 1].astype(bf16)).astype(f32)
    return jnp.stack([a0, b0], axis=1)


def fold(v):
    return fold_last(fold_first(v[None]))[0]


def ring_gather(v):
    got = [v]
    for _ in range(lax.axis_size("sq") - 1):
        got.append(shift(got[-1], 1))
    return got


def ring_scatter(parts):
    moving = parts[1]
    for t in list(range(2, len(parts))) + [0]:
        got = shift(moving.astype(bf16), 1)
        moving = parts[t].astype(f32) + got.astype(f32)
    return moving


def pull_kernel(pick, *refs):
    *pieces, main, grads, tail, select = refs
    groups, slots, depth = select.shape
    n = len(pieces) // groups
    width = main.shape[-1]
    capacity = slots // (depth // BLOCK)
    place = lax.broadcasted_iota(jnp.int32, (1, depth), 1) // BLOCK
    place = (place * 128).astype(f32)
    ids = lax.broadcasted_iota(jnp.int32, (slots, 1), 0)
    ids = ((ids // capacity) * 128 + ids % capacity + 1).astype(f32)
    for g in range(groups):
        mine = pieces[g * n : (g + 1) * n]
        last = jnp.concatenate([piece[:, pl.ds(2 * width, 128)] for piece in mine], axis=0)
        code = dot_nt(pick[...], last)[:1]
        kept = (code > 0.0) & (code <= capacity)
        code = jnp.where(kept, code + place, -1.0)
        chosen = jnp.where(code == ids, 1.0, 0.0).astype(bf16)
        select[g] = chosen
        at = pl.ds(g * slots, slots)
        for out, first in ((main, 0), (grads, width)):
            rows = [piece[:, pl.ds(first, width)] for piece in mine]
            rows = jnp.concatenate(rows, axis=0)
            out[at, :] = dot(chosen, rows).astype(bf16)
        tail[at, :] = dot(chosen, last).astype(bf16)


def pull_pieces(pick, pieces, groups, capacity, width):
    depth = len(pieces) // groups * pieces[0].shape[0]
    slots = depth // BLOCK * capacity
    shapes = [(groups * slots, width), (groups * slots, width), (groups * slots, 128)]
    shapes.append((groups, slots, depth))
    return pl.pallas_call(
        pull_kernel,
        out_shape=tuple(jax.ShapeDtypeStruct(shape, bf16) for shape in shapes),
        name="pull",
    )(pick, *pieces)


def on_device(
    tokens,
    segment_ids,
    routes,
    cotangent,
    q_weight,
    k_weight,
    v_weight,
    o_weight,
    router_weight,
    norm_gains,
    gate_up_weight,
    down_weight,
):
    n_dp, n_sq, n_cl = lax.axis_size("dp"), lax.axis_size("sq"), lax.axis_size("cl")
    dp, zi, cl = lax.axis_index("dp"), lax.axis_index("sq"), lax.axis_index("cl")
    nl, bl, width = tokens.shape
    rows = nl * bl
    n_ctx = n_sq * n_cl
    length = bl * n_ctx
    n_all = n_dp * n_ctx
    tp = n_cl * n_dp
    experts = n_ctx
    expert = zi * n_cl + cl
    capacity = max(2, (5 * bl * TOPK + 4 * experts - 1) // (4 * experts))
    ff = down_weight.shape[1]
    heads = H // tp
    hw = heads * HD
    kvw = 2 * HD // n_dp
    pack = hw + kvw
    score_scale = HD ** (-0.5)
    shard = width // n_all

    hit = jnp.any(
        routes[:, :, :, None] == jnp.arange(experts, dtype=jnp.int32), axis=2
    ).astype(bf16)
    below = jnp.tril(jnp.ones((bl, bl), bf16), -1)
    earlier = jnp.einsum("pq,jqe->jpe", below, hit, preferred_element_type=f32)
    codes = jnp.where(hit > 0, jnp.minimum(earlier + 1.0, capacity + 1.0), 0.0).astype(bf16)
    codes = jnp.pad(codes, ((0, 0), (0, 0), (0, 128 - experts)))

    small = jnp.concatenate(
        [router_weight.T.reshape(-1), norm_gains.reshape(-1)]
    )
    n_small = small.shape[0]
    n_router = experts * shard
    small = jnp.pad(small, (0, -n_small % 128)).reshape(-1, 128)
    kv_weight = jnp.concatenate(
        [k_weight.reshape(shard, n_cl, HD), v_weight.reshape(shard, n_cl, HD)], axis=-1
    )
    packed = jnp.concatenate(
        [
            q_weight.reshape(shard, n_cl, n_dp, hw),
            kv_weight.reshape(shard, n_cl, n_dp, kvw),
        ],
        axis=-1,
    )
    packed = jnp.transpose(packed, (1, 2, 0, 3)).reshape(tp, shard, pack)
    packed = lax.all_to_all(packed, ("cl", "dp"), split_axis=0, concat_axis=0, tiled=True)
    packed = jnp.transpose(packed.reshape(n_cl, n_dp, shard, pack), (1, 0, 2, 3))
    gu_full = dp_gather(gate_up_weight[0]).reshape(width, 2 * ff)
    down_full = jnp.concatenate(list(dp_gather(down_weight[0])), axis=1)

    packed, small = tie(packed, small)
    small = every_gather(small).reshape(n_all, -1)
    router_t = small[:, :n_router].reshape(n_all, experts, shard)
    router_t = jnp.transpose(router_t, (1, 0, 2)).reshape(experts, width)
    gains = small[:, n_router:n_small].reshape(-1).astype(f32)
    attn_gain = gains[:width]
    ffn_gain = gains[width : 2 * width]
    q_gain = gains[2 * width : 2 * width + HD]
    k_gain = gains[2 * width + HD :]

    qkv_w = jnp.zeros((n_dp, n_sq, n_cl, shard, pack), bf16)
    rank = cl * n_dp + dp
    qkv_pieces = [packed, shift(packed, 1)]
    inputs_low = to_sequence(tokens).reshape(rows, width)
    upstream_low = jnp.concatenate([cotangent, codes], axis=-1)
    upstream_low = to_sequence(upstream_low).reshape(rows, -1)
    qkv_pieces[1], inputs_low, upstream_low = tie(qkv_pieces[1], inputs_low, upstream_low)
    inputs = inputs_low.astype(f32)
    inputs_all = spread(inputs_low)
    for _ in range(2, n_sq - 1):
        qkv_pieces.append(shift(qkv_pieces[-1], 1))
    qkv_pieces[-1], inputs_all, gu_full, down_full, o_weight, upstream_low = tie(
        qkv_pieces[-1], inputs_all, gu_full, down_full, o_weight, upstream_low
    )
    upstream = upstream_low[:, :width].astype(f32)
    own_codes = upstream_low[:, width : width + experts].astype(f32)
    qkv_pieces.append(shift(qkv_pieces[-1], 1))
    o_mine = lax.ppermute(o_weight, ("dp", "sq", "cl"), head_pairs())
    inputs_all = dp_rows(jnp.concatenate(inputs_all)).reshape(length, width).astype(f32)

    for t, piece in enumerate(qkv_pieces):
        qkv_w = lax.dynamic_update_index_in_dim(qkv_w, piece, (zi - t) % n_sq, 1)
    qkv_w = qkv_w.reshape(width, pack)

    order = jnp.array([[0, 1, 2, 3], [0, 2, 1, 3]], jnp.int32)
    chip_of = order ^ cl
    hb = nl // 2
    block_of = (zi - jnp.arange(nl).reshape(2, hb)) % nl
    d_ids = (jnp.arange(n_dp) ^ dp)[:, None, None, None]
    block_ids = (d_ids * nl + block_of[None, :, None, :]) * n_cl + chip_of[None, :, :, None]
    positions = block_ids[..., None] * bl + jnp.arange(bl)
    positions = positions.reshape(length).astype(jnp.int32)
    segments = take(dp_gather(segment_ids).reshape(n_dp * nl, length), zi)
    segments = segments.reshape(1, n_dp * nl * n_cl, bl)
    found = block_ids.reshape(-1, 1, 1) == jnp.arange(n_dp * nl * n_cl)[None, :, None]
    segments = jnp.sum(jnp.where(found, segments, 0), axis=1).reshape(length)
    cosine, sine_table = rope_tables(positions, HD)
    cosine, sine_table = cosine[:, None, :], sine_table[:, None, :]

    first_scale = rms_scale(inputs)
    normed_all = (inputs_all * rms_scale(inputs_all) * attn_gain).astype(bf16)
    proj = dot(normed_all, qkv_w)
    q_proj = proj[:, :hw].reshape(length, heads, HD)
    kv_proj = dp_columns(proj[:, hw:].reshape(n_dp, -1, kvw)).reshape(n_dp, length, kvw)
    kv_proj = jnp.concatenate(list(kv_proj), axis=-1)
    k_proj = kv_proj[:, None, :HD]
    values = kv_proj[:, HD:].astype(bf16)
    q_scale = rms_scale(q_proj)
    k_scale = rms_scale(k_proj)
    queries = rotate(q_proj * q_scale * q_gain, cosine, sine_table).astype(bf16)
    keys = rotate(k_proj * k_scale * k_gain, cosine, sine_table).astype(bf16)[:, 0]
    queries, o_mine = tie(queries, o_mine)
    o_pieces = [o_mine, shift(o_mine, 1)]
    values, o_pieces[1] = tie(values, o_pieces[1])
    for _ in range(2, n_sq):
        o_pieces.append(shift(o_pieces[-1], 1))
    allowed = (positions[None, :] <= positions[:, None]) & (
        segments[None, :] == segments[:, None]
    )
    scores = jnp.einsum("qhd,kd->hqk", queries, keys, preferred_element_type=f32) * score_scale
    scores = jnp.where(allowed[None], scores, neg_big)
    terms = jnp.exp(scores - jnp.max(scores, axis=-1, keepdims=True))
    probs = terms / jnp.sum(terms, axis=-1, keepdims=True)
    prob_low = probs.astype(bf16)
    attended = jnp.einsum("hqk,kd->qhd", prob_low, values, preferred_element_type=f32)
    attended = attended.reshape(length, hw).astype(bf16)
    attended, o_pieces[2] = tie(attended, o_pieces[2])
    o_full = jnp.zeros((n_sq,) + o_weight.shape, bf16)
    for t, piece in enumerate(o_pieces):
        o_full = lax.dynamic_update_index_in_dim(o_full, piece, (zi - t - rank) % n_sq, 0)
    o_full = o_full.reshape(hw, width)
    mixed = [dot(attended_m, o_full) for attended_m in attended.reshape(n_dp, -1, hw)]
    mixed = fold(dp_fold(mixed).reshape(2, n_cl, rows // 2, width)).reshape(rows, width)
    middle = inputs + mixed
    second_scale = rms_scale(middle)
    hidden = (middle * second_scale * ffn_gain).astype(bf16)
    logits = dot_nt(hidden, router_t)
    routed = own_codes > 0
    top = jnp.max(jnp.where(routed, logits, neg_big), axis=-1, keepdims=True)
    gate_terms = jnp.where(routed, jnp.exp(logits - top), 0.0)
    gates = gate_terms / jnp.sum(gate_terms, axis=-1, keepdims=True)
    gates_high = gates.astype(bf16)
    gates_low = (gates - gates_high.astype(f32)).astype(bf16)
    extra = jnp.concatenate([gates_high, gates_low, own_codes.astype(bf16)], axis=-1)
    extra = jnp.pad(extra, ((0, 0), (0, 128 - 3 * experts)))
    hidden_wide = jnp.concatenate([hidden, upstream_low[:, :width], extra], axis=-1)

    lanes = jnp.arange(128)
    half = rows // 2
    n_slot = n_cl * hb * capacity
    code_pick = jnp.broadcast_to(lanes == 2 * experts + expert, (8, 128)).astype(bf16)
    pick = (lanes == expert) | (lanes == experts + expert)

    def push(chosen, v):
        v = v.reshape(chosen.shape[:2] + (-1,))
        got = jnp.einsum("grt,grd->gtd", chosen, v, preferred_element_type=f32)
        return got.astype(bf16)

    per = 2
    n_chunk = n_sq // per
    ins, actives, out_grads, gu_grads, backs = [], [], [], [], []
    arrived = []
    moving = hidden_wide
    for t in range(n_sq):
        arrived += spread(moving)
        if t == 0:
            moving = shift(moving, 1)
        elif t + 1 < n_sq:
            moving = shift(moving, 1)
    for chunk in range(n_chunk):
        pieces = arrived[chunk * per * 8 : (chunk + 1) * per * 8]
        expert_in, grad_slot, gate_lanes, chosen = pull_pieces(
            code_pick, pieces, 2 * per, capacity, width
        )
        gate_slot = jnp.sum(
            jnp.where(pick, gate_lanes.astype(f32), 0.0), axis=-1, keepdims=True
        )
        grad_slot = grad_slot.astype(f32)
        gate_up = dot(expert_in, gu_full)
        gate_part, up_part = gate_up[:, :ff], gate_up[:, ff:]
        sigmoid_gate = jax.nn.sigmoid(gate_part)
        activated = (gate_part * sigmoid_gate * up_part).astype(bf16)
        if chunk:
            activated, back_first = tie(activated, back_first)
            backs += list(fold_last(back_first))
        expert_out = dot(activated, down_full).astype(bf16)
        out_wide = expert_out.astype(f32)
        pair_grad = jnp.sum(grad_slot * out_wide, axis=-1, keepdims=True)
        out_grad = (gate_slot * grad_slot).astype(bf16)
        act_grad = dot_nt(out_grad, down_full)
        gate_back = act_grad * up_part * sigmoid_gate * (1.0 + gate_part * (1.0 - sigmoid_gate))
        up_back = act_grad * gate_part * sigmoid_gate
        gu_grad = jnp.concatenate([gate_back, up_back], axis=-1).astype(bf16)
        if chunk:
            gu_grad, backs = tie(gu_grad, backs)
        row_grad = dot_nt(gu_grad, gu_full).astype(bf16)
        pair_high = pair_grad.astype(bf16)
        pair_low = (pair_grad - pair_high.astype(f32)).astype(bf16)
        pair_extra = jnp.where(
            lanes == expert, pair_high, jnp.where(lanes == experts + expert, pair_low, 0)
        ).astype(bf16)
        moe = (gate_slot * out_wide).astype(bf16)
        back = push(chosen, jnp.concatenate([row_grad, moe, pair_extra], axis=-1))
        if chunk + 1 < n_chunk:
            code_pick, back = tie(code_pick, back)
        back_first = fold_first(back.reshape(per, 2, n_cl, half, -1))
        ins.append(expert_in)
        actives.append(activated)
        out_grads.append(out_grad)
        gu_grads.append(gu_grad)
    gu_grad = jnp.concatenate(gu_grads)
    activated = jnp.concatenate(actives)

    def columns(parts, m):
        size = width // n_dp
        at = (dp ^ m) * size
        return jnp.concatenate([lax.dynamic_slice_in_dim(v, at, size, 1) for v in parts])

    gu_parts = [dot_tn(columns(ins, m), gu_grad) for m in range(n_dp)]
    down_parts = [dot_tn(activated, columns(out_grads, m)) for m in range(n_dp)]
    back_first, gu_parts, down_parts = tie(back_first, gu_parts, down_parts)
    backs = [v.reshape(rows, -1) for v in backs + list(fold_last(back_first))]
    back = ring_scatter(backs).astype(bf16).astype(f32)
    output = (middle + back[:, width : 2 * width]).astype(bf16)

    pair_own = back[:, 2 * width :]
    pair_own = pair_own[:, :experts] + pair_own[:, experts : 2 * experts]
    chosen_grad = gates * (pair_own - jnp.sum(gates * pair_own, axis=-1, keepdims=True))
    logit_grad = chosen_grad.astype(bf16)
    hidden_grad = back[:, :width] + dot(logit_grad, router_t)
    router_grad = dot_tn(logit_grad, hidden)
    ffn_gain_grad = jnp.sum(hidden_grad * middle * second_scale, axis=0)
    middle_grad = upstream + norm_back(middle, second_scale, ffn_gain, hidden_grad)

    middle_low = dp_rows(jnp.concatenate(spread(middle_grad.astype(bf16)))).reshape(length, width)
    output = from_sequence(output.reshape(nl, bl, width))
    middle_low, output = tie(middle_low, output)
    o_grad = dot_tn(attended, middle_low).reshape(n_sq, -1, width)
    attended_grad = dot_nt(middle_low, o_full).astype(bf16).reshape(length, heads, HD)
    attended_grad, o_grad = tie(attended_grad, o_grad)
    o_parts = [take(o_grad, (zi - t - rank) % n_sq) for t in range(n_sq)]
    o_got = [shift(o_parts[t].astype(bf16), -t) for t in range(1, n_sq)]
    prob_grad = jnp.einsum("qhd,kd->hqk", attended_grad, values, preferred_element_type=f32)
    inner_sum = jnp.sum(probs * prob_grad, axis=-1, keepdims=True)
    score_grad = (probs * (prob_grad - inner_sum)).astype(bf16)
    value_part = jnp.einsum("hqk,qhd->kd", prob_low, attended_grad, preferred_element_type=f32)
    key_part = (
        jnp.einsum("hqk,qhd->kd", score_grad, queries, preferred_element_type=f32) * score_scale
    )
    query_grad = (
        jnp.einsum("hqk,kd->qhd", score_grad, keys, preferred_element_type=f32) * score_scale
    )
    kv_sum = jnp.concatenate([key_part, value_part], axis=-1).reshape(n_dp, -1, 2 * HD)
    kv_sum = dp_sum(kv_sum).reshape(length, 2 * HD)
    query_grad, o_got = tie(query_grad, o_got)
    o_got = o_parts[0].astype(f32) + sum(v.astype(f32) for v in o_got)
    o_share = lax.ppermute(
        o_got.astype(bf16), ("dp", "sq", "cl"), [(b, a) for a, b in head_pairs()]
    )
    key_rot_grad = rotate_back(kv_sum[:, None, :HD], cosine, sine_table)
    k_gain_grad = jnp.sum(key_rot_grad * k_proj * k_scale, axis=(0, 1))
    k_gain_grad = jnp.where(dp == 0, k_gain_grad, 0.0)
    k_low = norm_back(k_proj, k_scale, k_gain, key_rot_grad)[:, 0].astype(bf16)
    kv_low = jnp.concatenate([k_low, kv_sum[:, HD:].astype(bf16)], axis=-1)
    kv_low = lax.dynamic_slice_in_dim(kv_low, dp * kvw, kvw, 1)
    query_rot_grad = rotate_back(query_grad, cosine, sine_table)
    q_gain_grad = jnp.sum(query_rot_grad * q_proj * q_scale, axis=(0, 1))
    q_low = norm_back(q_proj, q_scale, q_gain, query_rot_grad).reshape(length, hw).astype(bf16)
    qkv_low = jnp.concatenate([q_low, kv_low], axis=-1)
    qkv_low, gu_parts, down_parts = tie(qkv_low, gu_parts, down_parts)
    gu_share, down_share = dp_fold(gu_parts), dp_fold(down_parts)
    w_grad = dot_tn(normed_all, qkv_low).reshape(n_dp, n_sq, n_cl, shard, pack)
    w_parts = [take(w_grad, (zi - t) % n_sq, 1) for t in range(n_sq)]
    w_got = [shift(w_parts[t].astype(bf16), -t) for t in range(1, n_sq)]
    normed_grad = [dot_nt(low_m, qkv_w) for low_m in qkv_low.reshape(n_dp, -1, pack)]
    normed_first = fold_first(dp_fold(normed_grad).reshape(1, 2, n_cl, rows // 2, width))
    normed_grad = fold_last(normed_first).reshape(rows, width)
    normed_grad, w_got, gu_share, down_share = tie(normed_grad, w_got, gu_share, down_share)
    w_got = w_parts[0].astype(f32) + sum(v.astype(f32) for v in w_got)
    attn_gain_grad = jnp.sum(normed_grad * inputs * first_scale, axis=0)
    input_grad = middle_grad + norm_back(inputs, first_scale, attn_gain, normed_grad)
    input_grad = from_sequence(input_grad.astype(bf16).reshape(nl, bl, width))

    w_got, o_share = tie(w_got, o_share)
    o_share = o_share.astype(f32)
    w_grad = w_got.astype(bf16)
    w_grad = jnp.transpose(w_grad, (1, 0, 2, 3)).reshape(tp, shard, pack)
    w_grad = lax.all_to_all(w_grad, ("cl", "dp"), split_axis=0, concat_axis=0, tiled=True)
    w_grad = jnp.transpose(w_grad.reshape(n_cl, n_dp, shard, pack), (2, 0, 1, 3)).astype(f32)
    q_share = w_grad[..., :hw].reshape(shard, -1)
    kv_share = w_grad[..., hw:].reshape(shard, n_cl, 2 * HD)
    k_share = kv_share[..., :HD].reshape(shard, -1)
    v_share = kv_share[..., HD:].reshape(shard, -1)

    gain_grads = jnp.concatenate([attn_gain_grad, ffn_gain_grad, q_gain_grad, k_gain_grad])
    router_grad = jnp.transpose(router_grad.reshape(experts, n_all, shard), (1, 0, 2))
    small_grad = jnp.concatenate(
        [router_grad.reshape(n_all, n_router), gain_grads.reshape(n_all, -1)], axis=-1
    )
    small_grad = jnp.pad(small_grad, ((0, 0), (0, -n_small % 128))).reshape(n_all, -1, 128)
    small_grad = every_scatter(small_grad).reshape(-1)
    router_share = small_grad[:n_router].reshape(experts, shard).T
    gains_share = small_grad[n_router:n_small]
    return (
        output,
        input_grad,
        q_share,
        k_share,
        v_share,
        o_share,
        router_share,
        gains_share,
        gu_share[None],
        down_share[None],
    )


def solution(mesh):
    n_dp, n_ctx = mesh.devices.shape
    n_cl = KV
    fine = Mesh(mesh.devices.reshape(n_dp, n_ctx // n_cl, n_cl), ("dp", "sq", "cl"))
    ctx = ("sq", "cl")
    every = ("dp", "sq", "cl")
    rows = P("dp", ctx, None)
    placed = (
        rows,
        P("dp", None),
        rows,
        rows,
        P(every, None),
        P(every, None),
        P(every, None),
        P(every, None),
        P(every, None),
        P(every),
        P(ctx, "dp", None),
        P(ctx, None, "dp"),
    )
    return jax.shard_map(
        on_device,
        mesh=fine,
        in_specs=placed,
        out_specs=(
            rows,
            rows,
            P(every, None),
            P(every, None),
            P(every, None),
            P(every, None),
            P(every, None),
            P(every),
            P(ctx, "dp", None),
            P(ctx, None, "dp"),
        ),
        check_vma=False,
    )
```

```python
import jax
import jax.numpy as jnp
from jax import lax
from jax.experimental import pallas as pl
from jax.sharding import Mesh, PartitionSpec as P

H = 32
KV = 4
HD = 128
TOPK = 8
BLOCK = 64

eps_norm = 1e-06
rope_base = 1000000.0
neg_big = -1e30
f32 = jnp.float32
bf16 = jnp.bfloat16


def tie(*v):
    return lax.optimization_barrier(v)


def rms_scale(operand):
    return lax.rsqrt(jnp.mean(operand * operand, axis=-1, keepdims=True) + eps_norm)


def norm_back(operand, scale_rows, gain_vec, upstream):
    weighted = gain_vec * upstream
    inner_mean = jnp.mean(operand * weighted, axis=-1, keepdims=True)
    return scale_rows * weighted - operand * scale_rows * scale_rows * scale_rows * inner_mean


def rope_tables(positions, head_size):
    frequency = rope_base ** (-(jnp.arange(head_size // 2, dtype=f32) * 2.0 / head_size))
    angles = positions.astype(f32)[:, None] * frequency[None, :]
    angles = jnp.concatenate([angles, angles], axis=-1)
    return (jnp.cos(angles), jnp.sin(angles))


def rotate(operand, cosine, sine_table):
    half_width = operand.shape[-1] // 2
    turned = jnp.concatenate([-operand[..., half_width:], operand[..., :half_width]], axis=-1)
    return operand * cosine + turned * sine_table


def rotate_back(upstream, cosine, sine_table):
    shifted = upstream * sine_table
    half_width = upstream.shape[-1] // 2
    return upstream * cosine + jnp.concatenate(
        [shifted[..., half_width:], -shifted[..., :half_width]], axis=-1
    )


def dot(a, b):
    return jnp.dot(a, b, preferred_element_type=f32)


def dot_nt(a, b):
    return lax.dot_general(a, b, (((1,), (1,)), ((), ())), preferred_element_type=f32)


def dot_tn(a, b):
    return lax.dot_general(a, b, (((0,), (0,)), ((), ())), preferred_element_type=f32)


def take(v, index, axis=0):
    return lax.dynamic_index_in_dim(v, index, axis, keepdims=False)


def flip(v, axis, bit):
    n = lax.axis_size(axis)
    return lax.ppermute(v, axis, [(i, i ^ bit) for i in range(n)])


def px(v):
    return flip(v, "cl", 1)


def py(v):
    return flip(v, "cl", 2)


def shift(v, by):
    n = lax.axis_size("sq")
    return lax.ppermute(v, "sq", [(i, (i + by) % n) for i in range(n)])


def bits_of(axis):
    n, bit, out = lax.axis_size(axis), 1, []
    while bit < n:
        out.append(bit)
        bit *= 2
    return out


def every_gather(v):
    n = lax.axis_size("dp") * lax.axis_size("sq") * lax.axis_size("cl")
    v = jnp.broadcast_to(v[None], (n,) + v.shape)
    return lax.all_to_all(v, ("dp", "sq", "cl"), split_axis=0, concat_axis=0, tiled=True)


def every_scatter(v):
    v = lax.all_to_all(v, ("dp", "sq", "cl"), split_axis=0, concat_axis=0, tiled=True)
    return jnp.sum(v, axis=0)


def xor_groups(v, bit):
    rest = v.shape[1:]
    v = v.reshape((-1, 2, bit) + rest)
    return jnp.concatenate([v[:, 1:], v[:, :1]], axis=1).reshape((-1,) + rest)


def dp_gather(v):
    v = v[None]
    index = lax.axis_index("dp")
    for bit in bits_of("dp"):
        other = flip(v, "dp", bit)
        upper = (index & bit) != 0
        v = jnp.concatenate([jnp.where(upper, other, v), jnp.where(upper, v, other)], axis=0)
    return v


def dp_columns(v):
    v = v[None]
    index = lax.axis_index("dp")
    for bit in bits_of("dp"):
        other = flip(v, "dp", bit)
        other = jnp.swapaxes(xor_groups(jnp.swapaxes(other, 0, 1), bit), 0, 1)
        upper = (index & bit) != 0
        v = jnp.concatenate([jnp.where(upper, other, v), jnp.where(upper, v, other)], axis=0)
    return v


def dp_rows(v):
    v = v[None]
    for bit in bits_of("dp"):
        v = jnp.concatenate([v, flip(v, "dp", bit)], axis=0)
    return v


def dp_fold(parts):
    for bit in reversed(bits_of("dp")):
        parts = [
            parts[m].astype(f32) + flip(parts[m + bit].astype(bf16), "dp", bit).astype(f32)
            for m in range(bit)
        ]
    return parts[0]


def dp_sum(v):
    for bit in bits_of("dp"):
        v = v + xor_groups(flip(v.astype(bf16), "dp", bit), bit).astype(f32)
    return v


def to_sequence(v):
    nl, n_dp, n_sq = v.shape[0], lax.axis_size("dp"), lax.axis_size("sq")
    zi = lax.axis_index("sq")
    got = []
    for m in range(nl):
        pairs = [
            (d * n_sq + z, (z // nl) * n_sq + nl * d + (m + z) % nl)
            for d in range(n_dp)
            for z in range(n_sq)
        ]
        got.append(lax.ppermute(take(v, (m + zi) % nl), ("dp", "sq"), pairs))
    return jnp.stack(got)


def from_sequence(v):
    nl, n_dp, n_sq = v.shape[0], lax.axis_size("dp"), lax.axis_size("sq")
    zi = lax.axis_index("sq")
    got = []
    for m in range(nl):
        pairs = [
            ((z // nl) * n_sq + nl * d + (m + z) % nl, d * n_sq + z)
            for d in range(n_dp)
            for z in range(n_sq)
        ]
        got.append(lax.ppermute(v[m], ("dp", "sq"), pairs))
    got = jnp.stack(got)
    return jnp.stack([take(got, (j - zi) % nl) for j in range(nl)])


def head_pairs():
    n_dp, n_sq, n_cl = lax.axis_size("dp"), lax.axis_size("sq"), lax.axis_size("cl")
    pairs = []
    for f in range(n_dp * n_sq * n_cl):
        r, q = f // n_sq, f % n_sq
        pairs.append((f, ((r % n_dp) * n_sq + (q + r) % n_sq) * n_cl + r // n_dp))
    return pairs


def spread(v):
    h = v.shape[0] // 2
    a, b = v[:h], v[h:]
    a1, b1 = px(a), py(b)
    a2, b2 = py(a), px(b)
    a3, b3 = py(a1), px(b1)
    return [a, a1, a2, a3, b, b1, b2, b3]


def fold_first(v):
    ra, rb = py(v[:, 0, 2:].astype(bf16)), px(v[:, 1, 2:].astype(bf16))
    return v[:, :, :2], ra, rb


def fold_last(first):
    v, ra, rb = first
    a = v[:, 0].astype(f32) + ra.astype(f32)
    b = v[:, 1].astype(f32) + rb.astype(f32)
    a0 = a[:, 0] + px(a[:, 1].astype(bf16)).astype(f32)
    b0 = b[:, 0] + py(b[:, 1].astype(bf16)).astype(f32)
    return jnp.stack([a0, b0], axis=1)


def fold(v):
    return fold_last(fold_first(v[None]))[0]


def ring_gather(v):
    got = [v]
    for _ in range(lax.axis_size("sq") - 1):
        got.append(shift(got[-1], 1))
    return got


def ring_scatter(parts):
    moving = parts[1]
    for t in list(range(2, len(parts))) + [0]:
        got = shift(moving.astype(bf16), 1)
        moving = parts[t].astype(f32) + got.astype(f32)
    return moving


def pull_kernel(pick, *refs):
    *pieces, main, grads, tail, select = refs
    groups, slots, depth = select.shape
    n = len(pieces) // groups
    width = main.shape[-1]
    capacity = slots // (depth // BLOCK)
    place = lax.broadcasted_iota(jnp.int32, (1, depth), 1) // BLOCK
    place = (place * 128).astype(f32)
    ids = lax.broadcasted_iota(jnp.int32, (slots, 1), 0)
    ids = ((ids // capacity) * 128 + ids % capacity + 1).astype(f32)
    for g in range(groups):
        mine = pieces[g * n : (g + 1) * n]
        last = jnp.concatenate([piece[:, pl.ds(2 * width, 128)] for piece in mine], axis=0)
        code = dot_nt(pick[...], last)[:1]
        kept = (code > 0.0) & (code <= capacity)
        code = jnp.where(kept, code + place, -1.0)
        chosen = jnp.where(code == ids, 1.0, 0.0).astype(bf16)
        select[g] = chosen
        at = pl.ds(g * slots, slots)
        for out, first in ((main, 0), (grads, width)):
            rows = [piece[:, pl.ds(first, width)] for piece in mine]
            rows = jnp.concatenate(rows, axis=0)
            out[at, :] = dot(chosen, rows).astype(bf16)
        tail[at, :] = dot(chosen, last).astype(bf16)


def pull_pieces(pick, pieces, groups, capacity, width):
    depth = len(pieces) // groups * pieces[0].shape[0]
    slots = depth // BLOCK * capacity
    shapes = [(groups * slots, width), (groups * slots, width), (groups * slots, 128)]
    shapes.append((groups, slots, depth))
    return pl.pallas_call(
        pull_kernel,
        out_shape=tuple(jax.ShapeDtypeStruct(shape, bf16) for shape in shapes),
        name="pull",
    )(pick, *pieces)


def on_device(
    tokens,
    segment_ids,
    routes,
    cotangent,
    q_weight,
    k_weight,
    v_weight,
    o_weight,
    router_weight,
    norm_gains,
    gate_up_weight,
    down_weight,
):
    n_dp, n_sq, n_cl = lax.axis_size("dp"), lax.axis_size("sq"), lax.axis_size("cl")
    dp, zi, cl = lax.axis_index("dp"), lax.axis_index("sq"), lax.axis_index("cl")
    nl, bl, width = tokens.shape
    rows = nl * bl
    n_ctx = n_sq * n_cl
    length = bl * n_ctx
    n_all = n_dp * n_ctx
    tp = n_cl * n_dp
    experts = n_ctx
    expert = zi * n_cl + cl
    capacity = max(2, (5 * bl * TOPK + 4 * experts - 1) // (4 * experts))
    ff = down_weight.shape[1]
    heads = H // tp
    hw = heads * HD
    kvw = 2 * HD // n_dp
    pack = hw + kvw
    score_scale = HD ** (-0.5)
    shard = width // n_all

    hit = jnp.any(
        routes[:, :, :, None] == jnp.arange(experts, dtype=jnp.int32), axis=2
    ).astype(bf16)
    below = jnp.tril(jnp.ones((bl, bl), bf16), -1)
    earlier = jnp.einsum("pq,jqe->jpe", below, hit, preferred_element_type=f32)
    codes = jnp.where(hit > 0, jnp.minimum(earlier + 1.0, capacity + 1.0), 0.0).astype(bf16)
    codes = jnp.pad(codes, ((0, 0), (0, 0), (0, 128 - experts)))

    small = jnp.concatenate(
        [router_weight.T.reshape(-1), norm_gains.reshape(-1)]
    )
    n_small = small.shape[0]
    n_router = experts * shard
    small = jnp.pad(small, (0, -n_small % 128)).reshape(-1, 128)
    kv_weight = jnp.concatenate(
        [k_weight.reshape(shard, n_cl, HD), v_weight.reshape(shard, n_cl, HD)], axis=-1
    )
    packed = jnp.concatenate(
        [
            q_weight.reshape(shard, n_cl, n_dp, hw),
            kv_weight.reshape(shard, n_cl, n_dp, kvw),
        ],
        axis=-1,
    )
    packed = jnp.transpose(packed, (1, 2, 0, 3)).reshape(tp, shard, pack)
    packed = lax.all_to_all(packed, ("cl", "dp"), split_axis=0, concat_axis=0, tiled=True)
    packed = jnp.transpose(packed.reshape(n_cl, n_dp, shard, pack), (1, 0, 2, 3))
    gu_full = dp_gather(gate_up_weight[0]).reshape(width, 2 * ff)
    down_full = jnp.concatenate(list(dp_gather(down_weight[0])), axis=1)

    packed, small = tie(packed, small)
    small = every_gather(small)
    qkv_w = jnp.zeros((n_dp, n_sq, n_cl, shard, pack), bf16)
    rank = cl * n_dp + dp
    qkv_pieces = [packed, shift(packed, 1)]
    inputs_low = to_sequence(tokens).reshape(rows, width)
    upstream_low = jnp.concatenate([cotangent, codes], axis=-1)
    qkv_pieces[1], inputs_low = tie(qkv_pieces[1], inputs_low)
    inputs = inputs_low.astype(f32)
    inputs_all = spread(inputs_low)
    for _ in range(2, n_sq - 1):
        qkv_pieces.append(shift(qkv_pieces[-1], 1))
    qkv_pieces[-1], inputs_all, o_weight, small = tie(
        qkv_pieces[-1], inputs_all, o_weight, small
    )
    small = small.reshape(n_all, -1)
    router_t = small[:, :n_router].reshape(n_all, experts, shard)
    router_t = jnp.transpose(router_t, (1, 0, 2)).reshape(experts, width)
    gains = small[:, n_router:n_small].reshape(-1).astype(f32)
    attn_gain = gains[:width]
    ffn_gain = gains[width : 2 * width]
    q_gain = gains[2 * width : 2 * width + HD]
    k_gain = gains[2 * width + HD :]
    qkv_pieces.append(shift(qkv_pieces[-1], 1))
    qkv_pieces[-1], gu_full, down_full, upstream_low = tie(
        qkv_pieces[-1], gu_full, down_full, upstream_low
    )
    upstream_low = to_sequence(upstream_low).reshape(rows, -1)
    upstream = upstream_low[:, :width].astype(f32)
    own_codes = upstream_low[:, width : width + experts].astype(f32)
    o_mine = lax.ppermute(o_weight, ("dp", "sq", "cl"), head_pairs())
    inputs_all = dp_rows(jnp.concatenate(inputs_all)).reshape(length, width).astype(f32)

    for t, piece in enumerate(qkv_pieces):
        qkv_w = lax.dynamic_update_index_in_dim(qkv_w, piece, (zi - t) % n_sq, 1)
    qkv_w = qkv_w.reshape(width, pack)

    order = jnp.array([[0, 1, 2, 3], [0, 2, 1, 3]], jnp.int32)
    chip_of = order ^ cl
    hb = nl // 2
    block_of = (zi - jnp.arange(nl).reshape(2, hb)) % nl
    d_ids = (jnp.arange(n_dp) ^ dp)[:, None, None, None]
    block_ids = (d_ids * nl + block_of[None, :, None, :]) * n_cl + chip_of[None, :, :, None]
    positions = block_ids[..., None] * bl + jnp.arange(bl)
    positions = positions.reshape(length).astype(jnp.int32)
    segments = take(dp_gather(segment_ids).reshape(n_dp * nl, length), zi)
    segments = segments.reshape(1, n_dp * nl * n_cl, bl)
    found = block_ids.reshape(-1, 1, 1) == jnp.arange(n_dp * nl * n_cl)[None, :, None]
    segments = jnp.sum(jnp.where(found, segments, 0), axis=1).reshape(length)
    cosine, sine_table = rope_tables(positions, HD)
    cosine, sine_table = cosine[:, None, :], sine_table[:, None, :]

    first_scale = rms_scale(inputs)
    normed_all = (inputs_all * rms_scale(inputs_all) * attn_gain).astype(bf16)
    proj = dot(normed_all, qkv_w)
    q_proj = proj[:, :hw].reshape(length, heads, HD)
    kv_proj = dp_columns(proj[:, hw:].reshape(n_dp, -1, kvw)).reshape(n_dp, length, kvw)
    kv_proj = jnp.concatenate(list(kv_proj), axis=-1)
    k_proj = kv_proj[:, None, :HD]
    values = kv_proj[:, HD:].astype(bf16)
    q_scale = rms_scale(q_proj)
    k_scale = rms_scale(k_proj)
    queries = rotate(q_proj * q_scale * q_gain, cosine, sine_table).astype(bf16)
    keys = rotate(k_proj * k_scale * k_gain, cosine, sine_table).astype(bf16)[:, 0]
    queries, o_mine = tie(queries, o_mine)
    o_pieces = [o_mine, shift(o_mine, 1)]
    values, o_pieces[1] = tie(values, o_pieces[1])
    for _ in range(2, n_sq):
        o_pieces.append(shift(o_pieces[-1], 1))
    allowed = (positions[None, :] <= positions[:, None]) & (
        segments[None, :] == segments[:, None]
    )
    scores = jnp.einsum("qhd,kd->hqk", queries, keys, preferred_element_type=f32) * score_scale
    scores = jnp.where(allowed[None], scores, neg_big)
    terms = jnp.exp(scores - jnp.max(scores, axis=-1, keepdims=True))
    probs = terms / jnp.sum(terms, axis=-1, keepdims=True)
    prob_low = probs.astype(bf16)
    attended = jnp.einsum("hqk,kd->qhd", prob_low, values, preferred_element_type=f32)
    attended = attended.reshape(length, hw).astype(bf16)
    attended, o_pieces[2] = tie(attended, o_pieces[2])
    o_full = jnp.zeros((n_sq,) + o_weight.shape, bf16)
    for t, piece in enumerate(o_pieces):
        o_full = lax.dynamic_update_index_in_dim(o_full, piece, (zi - t - rank) % n_sq, 0)
    o_full = o_full.reshape(hw, width)
    mixed = [dot(attended_m, o_full) for attended_m in attended.reshape(n_dp, -1, hw)]
    mixed = fold(dp_fold(mixed).reshape(2, n_cl, rows // 2, width)).reshape(rows, width)
    middle = inputs + mixed
    second_scale = rms_scale(middle)
    hidden = (middle * second_scale * ffn_gain).astype(bf16)
    logits = dot_nt(hidden, router_t)
    routed = own_codes > 0
    top = jnp.max(jnp.where(routed, logits, neg_big), axis=-1, keepdims=True)
    gate_terms = jnp.where(routed, jnp.exp(logits - top), 0.0)
    gates = gate_terms / jnp.sum(gate_terms, axis=-1, keepdims=True)
    gates_high = gates.astype(bf16)
    gates_low = (gates - gates_high.astype(f32)).astype(bf16)
    extra = jnp.concatenate([gates_high, gates_low, own_codes.astype(bf16)], axis=-1)
    extra = jnp.pad(extra, ((0, 0), (0, 128 - 3 * experts)))
    hidden_wide = jnp.concatenate([hidden, upstream_low[:, :width], extra], axis=-1)

    lanes = jnp.arange(128)
    half = rows // 2
    n_slot = n_cl * hb * capacity
    code_pick = jnp.broadcast_to(lanes == 2 * experts + expert, (8, 128)).astype(bf16)
    pick = (lanes == expert) | (lanes == experts + expert)

    def push(chosen, v):
        v = v.reshape(chosen.shape[:2] + (-1,))
        got = jnp.einsum("grt,grd->gtd", chosen, v, preferred_element_type=f32)
        return got.astype(bf16)

    per = 2
    n_chunk = n_sq // per
    ins, actives, out_grads, gu_grads, backs = [], [], [], [], []
    turns = list(range(1, n_sq)) + [0]
    arrived = [None] * n_sq
    moving, arrived[0] = tie(shift(hidden_wide, 1), spread(hidden_wide))
    for t in range(1, n_sq):
        arrived[t] = spread(moving)
        if t + 1 < n_sq:
            moving = shift(moving, 1)
    for chunk in range(n_chunk):
        pieces = sum([arrived[t] for t in turns[chunk * per : (chunk + 1) * per]], [])
        expert_in, grad_slot, gate_lanes, chosen = pull_pieces(
            code_pick, pieces, 2 * per, capacity, width
        )
        gate_slot = jnp.sum(
            jnp.where(pick, gate_lanes.astype(f32), 0.0), axis=-1, keepdims=True
        )
        grad_slot = grad_slot.astype(f32)
        gate_up = dot(expert_in, gu_full)
        gate_part, up_part = gate_up[:, :ff], gate_up[:, ff:]
        sigmoid_gate = jax.nn.sigmoid(gate_part)
        activated = (gate_part * sigmoid_gate * up_part).astype(bf16)
        if chunk:
            activated, back_first = tie(activated, back_first)
            backs += list(fold_last(back_first))
        expert_out = dot(activated, down_full).astype(bf16)
        out_wide = expert_out.astype(f32)
        pair_grad = jnp.sum(grad_slot * out_wide, axis=-1, keepdims=True)
        out_grad = (gate_slot * grad_slot).astype(bf16)
        act_grad = dot_nt(out_grad, down_full)
        gate_back = act_grad * up_part * sigmoid_gate * (1.0 + gate_part * (1.0 - sigmoid_gate))
        up_back = act_grad * gate_part * sigmoid_gate
        gu_grad = jnp.concatenate([gate_back, up_back], axis=-1).astype(bf16)
        if chunk:
            gu_grad, backs = tie(gu_grad, backs)
        row_grad = dot_nt(gu_grad, gu_full).astype(bf16)
        pair_high = pair_grad.astype(bf16)
        pair_low = (pair_grad - pair_high.astype(f32)).astype(bf16)
        pair_extra = jnp.where(
            lanes == expert, pair_high, jnp.where(lanes == experts + expert, pair_low, 0)
        ).astype(bf16)
        moe = (gate_slot * out_wide).astype(bf16)
        back = push(chosen, jnp.concatenate([row_grad, moe, pair_extra], axis=-1))
        if chunk + 1 < n_chunk:
            code_pick, back = tie(code_pick, back)
        back_first = fold_first(back.reshape(per, 2, n_cl, half, -1))
        ins.append(expert_in)
        actives.append(activated)
        out_grads.append(out_grad)
        gu_grads.append(gu_grad)
    gu_grad = jnp.concatenate(gu_grads)
    activated = jnp.concatenate(actives)

    def columns(parts, m):
        size = width // n_dp
        at = (dp ^ m) * size
        return jnp.concatenate([lax.dynamic_slice_in_dim(v, at, size, 1) for v in parts])

    gu_parts = [dot_tn(columns(ins, m), gu_grad) for m in range(n_dp)]
    down_parts = [dot_tn(activated, columns(out_grads, m)) for m in range(n_dp)]
    back_first, gu_parts, down_parts = tie(back_first, gu_parts, down_parts)
    backs = [v.reshape(rows, -1) for v in backs + list(fold_last(back_first))]
    back = ring_scatter(backs[-1:] + backs[:-1]).astype(bf16).astype(f32)
    output = (middle + back[:, width : 2 * width]).astype(bf16)

    pair_own = back[:, 2 * width :]
    pair_own = pair_own[:, :experts] + pair_own[:, experts : 2 * experts]
    chosen_grad = gates * (pair_own - jnp.sum(gates * pair_own, axis=-1, keepdims=True))
    logit_grad = chosen_grad.astype(bf16)
    hidden_grad = back[:, :width] + dot(logit_grad, router_t)
    router_grad = dot_tn(logit_grad, hidden)
    ffn_gain_grad = jnp.sum(hidden_grad * middle * second_scale, axis=0)
    middle_grad = upstream + norm_back(middle, second_scale, ffn_gain, hidden_grad)

    middle_low = dp_rows(jnp.concatenate(spread(middle_grad.astype(bf16)))).reshape(length, width)
    output = from_sequence(output.reshape(nl, bl, width))
    middle_low, output = tie(middle_low, output)
    o_grad = dot_tn(attended, middle_low).reshape(n_sq, -1, width)
    attended_grad = dot_nt(middle_low, o_full).astype(bf16).reshape(length, heads, HD)
    attended_grad, o_grad = tie(attended_grad, o_grad)
    o_parts = [take(o_grad, (zi - t - rank) % n_sq) for t in range(n_sq)]
    o_got = [shift(o_parts[t].astype(bf16), -t) for t in range(1, n_sq)]
    prob_grad = jnp.einsum("qhd,kd->hqk", attended_grad, values, preferred_element_type=f32)
    inner_sum = jnp.sum(probs * prob_grad, axis=-1, keepdims=True)
    score_grad = (probs * (prob_grad - inner_sum)).astype(bf16)
    value_part = jnp.einsum("hqk,qhd->kd", prob_low, attended_grad, preferred_element_type=f32)
    key_part = (
        jnp.einsum("hqk,qhd->kd", score_grad, queries, preferred_element_type=f32) * score_scale
    )
    query_grad = (
        jnp.einsum("hqk,kd->qhd", score_grad, keys, preferred_element_type=f32) * score_scale
    )
    kv_sum = jnp.concatenate([key_part, value_part], axis=-1).reshape(n_dp, -1, 2 * HD)
    kv_sum, o_got[:2] = tie(kv_sum, o_got[:2])
    kv_sum = dp_sum(kv_sum).reshape(length, 2 * HD)
    key_rot_grad = rotate_back(kv_sum[:, None, :HD], cosine, sine_table)
    k_gain_grad = jnp.sum(key_rot_grad * k_proj * k_scale, axis=(0, 1))
    k_gain_grad = jnp.where(dp == 0, k_gain_grad, 0.0)
    k_low = norm_back(k_proj, k_scale, k_gain, key_rot_grad)[:, 0].astype(bf16)
    kv_low = jnp.concatenate([k_low, kv_sum[:, HD:].astype(bf16)], axis=-1)
    kv_low = lax.dynamic_slice_in_dim(kv_low, dp * kvw, kvw, 1)
    query_rot_grad = rotate_back(query_grad, cosine, sine_table)
    q_gain_grad = jnp.sum(query_rot_grad * q_proj * q_scale, axis=(0, 1))
    q_low = norm_back(q_proj, q_scale, q_gain, query_rot_grad).reshape(length, hw).astype(bf16)
    qkv_low = jnp.concatenate([q_low, kv_low], axis=-1)
    qkv_low, gu_parts, down_parts = tie(qkv_low, gu_parts, down_parts)
    gu_share, down_share = dp_fold(gu_parts), dp_fold(down_parts)
    w_grad = dot_tn(qkv_low, normed_all)
    size = n_cl * shard

    def w_part(t):
        first = ((zi - t) % n_sq) * size
        parts = [
            lax.dynamic_slice_in_dim(w_grad, m * n_sq * size + first, size, 1)
            for m in range(n_dp)
        ]
        return jnp.concatenate(parts)

    w_grad, o_got[2:] = tie(w_grad, o_got[2:])
    w_got = [shift(w_part(t).astype(bf16), -t) for t in range(1, n_sq)]
    o_got = o_parts[0].astype(f32) + sum(v.astype(f32) for v in o_got)
    o_share = lax.ppermute(
        o_got.astype(bf16), ("dp", "sq", "cl"), [(b, a) for a, b in head_pairs()]
    )
    normed_grad = [dot_nt(low_m, qkv_w) for low_m in qkv_low.reshape(n_dp, -1, pack)]
    normed_first = fold_first(dp_fold(normed_grad).reshape(1, 2, n_cl, rows // 2, width))
    normed_grad = fold_last(normed_first).reshape(rows, width)
    normed_grad, w_got, gu_share, down_share = tie(normed_grad, w_got, gu_share, down_share)
    w_got = w_part(0) + sum(v.astype(f32) for v in w_got)
    attn_gain_grad = jnp.sum(normed_grad * inputs * first_scale, axis=0)
    input_grad = middle_grad + norm_back(inputs, first_scale, attn_gain, normed_grad)
    input_grad = from_sequence(input_grad.astype(bf16).reshape(nl, bl, width))

    w_got, o_share = tie(w_got, o_share)
    o_share = o_share.astype(f32)
    w_grad = w_got.astype(bf16).reshape(n_dp, pack, n_cl, shard)
    w_grad = jnp.transpose(w_grad, (2, 0, 3, 1)).reshape(tp, shard, pack)
    w_grad = lax.all_to_all(w_grad, ("cl", "dp"), split_axis=0, concat_axis=0, tiled=True)
    w_grad = jnp.transpose(w_grad.reshape(n_cl, n_dp, shard, pack), (2, 0, 1, 3)).astype(f32)
    q_share = w_grad[..., :hw].reshape(shard, -1)
    kv_share = w_grad[..., hw:].reshape(shard, n_cl, 2 * HD)
    k_share = kv_share[..., :HD].reshape(shard, -1)
    v_share = kv_share[..., HD:].reshape(shard, -1)

    gain_grads = jnp.concatenate([attn_gain_grad, ffn_gain_grad, q_gain_grad, k_gain_grad])
    router_grad = jnp.transpose(router_grad.reshape(experts, n_all, shard), (1, 0, 2))
    small_grad = jnp.concatenate(
        [router_grad.reshape(n_all, n_router), gain_grads.reshape(n_all, -1)], axis=-1
    )
    small_grad = jnp.pad(small_grad, ((0, 0), (0, -n_small % 128))).reshape(n_all, -1, 128)
    small_grad = every_scatter(small_grad).reshape(-1)
    router_share = small_grad[:n_router].reshape(experts, shard).T
    gains_share = small_grad[n_router:n_small]
    return (
        output,
        input_grad,
        q_share,
        k_share,
        v_share,
        o_share,
        router_share,
        gains_share,
        gu_share[None],
        down_share[None],
    )


def solution(mesh):
    n_dp, n_ctx = mesh.devices.shape
    n_cl = KV
    fine = Mesh(mesh.devices.reshape(n_dp, n_ctx // n_cl, n_cl), ("dp", "sq", "cl"))
    ctx = ("sq", "cl")
    every = ("dp", "sq", "cl")
    rows = P("dp", ctx, None)
    placed = (
        rows,
        P("dp", None),
        rows,
        rows,
        P(every, None),
        P(every, None),
        P(every, None),
        P(every, None),
        P(every, None),
        P(every),
        P(ctx, "dp", None),
        P(ctx, None, "dp"),
    )
    return jax.shard_map(
        on_device,
        mesh=fine,
        in_specs=placed,
        out_specs=(
            rows,
            rows,
            P(every, None),
            P(every, None),
            P(every, None),
            P(every, None),
            P(every, None),
            P(every),
            P(ctx, "dp", None),
            P(ctx, None, "dp"),
        ),
        check_vma=False,
    )
```

```python
import jax
import jax.numpy as jnp
from jax import lax
from jax.experimental import pallas as pl
from jax.sharding import Mesh, PartitionSpec as P

H = 32
KV = 4
HD = 128
TOPK = 8
BLOCK = 64

eps_norm = 1e-06
rope_base = 1000000.0
neg_big = -1e30
f32 = jnp.float32
bf16 = jnp.bfloat16


def tie(*v):
    return lax.optimization_barrier(v)


def rms_scale(operand):
    return lax.rsqrt(jnp.mean(operand * operand, axis=-1, keepdims=True) + eps_norm)


def norm_back(operand, scale_rows, gain_vec, upstream):
    weighted = gain_vec * upstream
    inner_mean = jnp.mean(operand * weighted, axis=-1, keepdims=True)
    return scale_rows * weighted - operand * scale_rows * scale_rows * scale_rows * inner_mean


def rope_tables(positions, head_size):
    frequency = rope_base ** (-(jnp.arange(head_size // 2, dtype=f32) * 2.0 / head_size))
    angles = positions.astype(f32)[:, None] * frequency[None, :]
    angles = jnp.concatenate([angles, angles], axis=-1)
    return (jnp.cos(angles), jnp.sin(angles))


def rotate(operand, cosine, sine_table):
    half_width = operand.shape[-1] // 2
    turned = jnp.concatenate([-operand[..., half_width:], operand[..., :half_width]], axis=-1)
    return operand * cosine + turned * sine_table


def rotate_back(upstream, cosine, sine_table):
    shifted = upstream * sine_table
    half_width = upstream.shape[-1] // 2
    return upstream * cosine + jnp.concatenate(
        [shifted[..., half_width:], -shifted[..., :half_width]], axis=-1
    )


def dot(a, b):
    return jnp.dot(a, b, preferred_element_type=f32)


def dot_nt(a, b):
    return lax.dot_general(a, b, (((1,), (1,)), ((), ())), preferred_element_type=f32)


def dot_tn(a, b):
    return lax.dot_general(a, b, (((0,), (0,)), ((), ())), preferred_element_type=f32)


def take(v, index, axis=0):
    return lax.dynamic_index_in_dim(v, index, axis, keepdims=False)


def flip(v, axis, bit):
    n = lax.axis_size(axis)
    return lax.ppermute(v, axis, [(i, i ^ bit) for i in range(n)])


def px(v):
    return flip(v, "cl", 1)


def py(v):
    return flip(v, "cl", 2)


def shift(v, by):
    n = lax.axis_size("sq")
    return lax.ppermute(v, "sq", [(i, (i + by) % n) for i in range(n)])


def bits_of(axis):
    n, bit, out = lax.axis_size(axis), 1, []
    while bit < n:
        out.append(bit)
        bit *= 2
    return out


def every_gather(v):
    n = lax.axis_size("dp") * lax.axis_size("sq") * lax.axis_size("cl")
    v = jnp.broadcast_to(v[None], (n,) + v.shape)
    return lax.all_to_all(v, ("dp", "sq", "cl"), split_axis=0, concat_axis=0, tiled=True)


def every_scatter(v):
    v = lax.all_to_all(v, ("dp", "sq", "cl"), split_axis=0, concat_axis=0, tiled=True)
    return jnp.sum(v, axis=0)


def xor_groups(v, bit):
    rest = v.shape[1:]
    v = v.reshape((-1, 2, bit) + rest)
    return jnp.concatenate([v[:, 1:], v[:, :1]], axis=1).reshape((-1,) + rest)


def dp_gather(v):
    v = v[None]
    index = lax.axis_index("dp")
    for bit in bits_of("dp"):
        other = flip(v, "dp", bit)
        upper = (index & bit) != 0
        v = jnp.concatenate([jnp.where(upper, other, v), jnp.where(upper, v, other)], axis=0)
    return v


def dp_columns(v):
    v = v[None]
    index = lax.axis_index("dp")
    for bit in bits_of("dp"):
        other = flip(v, "dp", bit)
        other = jnp.swapaxes(xor_groups(jnp.swapaxes(other, 0, 1), bit), 0, 1)
        upper = (index & bit) != 0
        v = jnp.concatenate([jnp.where(upper, other, v), jnp.where(upper, v, other)], axis=0)
    return v


def dp_rows(v):
    v = v[None]
    for bit in bits_of("dp"):
        v = jnp.concatenate([v, flip(v, "dp", bit)], axis=0)
    return v


def dp_fold(parts):
    for bit in reversed(bits_of("dp")):
        parts = [
            parts[m].astype(f32) + flip(parts[m + bit].astype(bf16), "dp", bit).astype(f32)
            for m in range(bit)
        ]
    return parts[0]


def dp_sum(v):
    for bit in bits_of("dp"):
        v = v + xor_groups(flip(v.astype(bf16), "dp", bit), bit).astype(f32)
    return v


def to_sequence(v):
    nl, n_dp, n_sq = v.shape[0], lax.axis_size("dp"), lax.axis_size("sq")
    zi = lax.axis_index("sq")
    got = []
    for m in range(nl):
        pairs = [
            (d * n_sq + z, (z // nl) * n_sq + nl * d + (m + z) % nl)
            for d in range(n_dp)
            for z in range(n_sq)
        ]
        got.append(lax.ppermute(take(v, (m + zi) % nl), ("dp", "sq"), pairs))
    return jnp.stack(got)


def from_sequence(v):
    nl, n_dp, n_sq = v.shape[0], lax.axis_size("dp"), lax.axis_size("sq")
    zi = lax.axis_index("sq")
    got = []
    for m in range(nl):
        pairs = [
            ((z // nl) * n_sq + nl * d + (m + z) % nl, d * n_sq + z)
            for d in range(n_dp)
            for z in range(n_sq)
        ]
        got.append(lax.ppermute(v[m], ("dp", "sq"), pairs))
    got = jnp.stack(got)
    return jnp.stack([take(got, (j - zi) % nl) for j in range(nl)])


def head_pairs():
    n_dp, n_sq, n_cl = lax.axis_size("dp"), lax.axis_size("sq"), lax.axis_size("cl")
    pairs = []
    for f in range(n_dp * n_sq * n_cl):
        r, q = f // n_sq, f % n_sq
        pairs.append((f, ((r % n_dp) * n_sq + (q + r) % n_sq) * n_cl + r // n_dp))
    return pairs


def spread(v):
    h = v.shape[0] // 2
    a, b = v[:h], v[h:]
    a1, b1 = px(a), py(b)
    a2, b2 = py(a), px(b)
    a3, b3 = py(a1), px(b1)
    return [a, a1, a2, a3, b, b1, b2, b3]


def fold_first(v):
    ra, rb = py(v[:, 0, 2:].astype(bf16)), px(v[:, 1, 2:].astype(bf16))
    return v[:, :, :2], ra, rb


def fold_last(first):
    v, ra, rb = first
    a = v[:, 0].astype(f32) + ra.astype(f32)
    b = v[:, 1].astype(f32) + rb.astype(f32)
    a0 = a[:, 0] + px(a[:, 1].astype(bf16)).astype(f32)
    b0 = b[:, 0] + py(b[:, 1].astype(bf16)).astype(f32)
    return jnp.stack([a0, b0], axis=1)


def fold(v):
    return fold_last(fold_first(v[None]))[0]


def ring_gather(v):
    got = [v]
    for _ in range(lax.axis_size("sq") - 1):
        got.append(shift(got[-1], 1))
    return got


def ring_scatter(parts):
    moving = parts[1]
    for t in list(range(2, len(parts))) + [0]:
        got = shift(moving.astype(bf16), 1)
        moving = parts[t].astype(f32) + got.astype(f32)
    return moving


def pull_kernel(pick, *refs):
    *pieces, main, grads, tail, select = refs
    groups, slots, depth = select.shape
    n = len(pieces) // groups
    width = main.shape[-1]
    capacity = slots // (depth // BLOCK)
    place = lax.broadcasted_iota(jnp.int32, (1, depth), 1) // BLOCK
    place = (place * 128).astype(f32)
    ids = lax.broadcasted_iota(jnp.int32, (slots, 1), 0)
    ids = ((ids // capacity) * 128 + ids % capacity + 1).astype(f32)
    for g in range(groups):
        mine = pieces[g * n : (g + 1) * n]
        last = jnp.concatenate([piece[:, pl.ds(2 * width, 128)] for piece in mine], axis=0)
        code = dot_nt(pick[...], last)[:1]
        kept = (code > 0.0) & (code <= capacity)
        code = jnp.where(kept, code + place, -1.0)
        chosen = jnp.where(code == ids, 1.0, 0.0).astype(bf16)
        select[g] = chosen
        at = pl.ds(g * slots, slots)
        for out, first in ((main, 0), (grads, width)):
            rows = [piece[:, pl.ds(first, width)] for piece in mine]
            rows = jnp.concatenate(rows, axis=0)
            out[at, :] = dot(chosen, rows).astype(bf16)
        tail[at, :] = dot(chosen, last).astype(bf16)


def pull_pieces(pick, pieces, groups, capacity, width):
    depth = len(pieces) // groups * pieces[0].shape[0]
    slots = depth // BLOCK * capacity
    shapes = [(groups * slots, width), (groups * slots, width), (groups * slots, 128)]
    shapes.append((groups, slots, depth))
    return pl.pallas_call(
        pull_kernel,
        out_shape=tuple(jax.ShapeDtypeStruct(shape, bf16) for shape in shapes),
        name="pull",
    )(pick, *pieces)


def on_device(
    tokens,
    segment_ids,
    routes,
    cotangent,
    q_weight,
    k_weight,
    v_weight,
    o_weight,
    router_weight,
    norm_gains,
    gate_up_weight,
    down_weight,
):
    n_dp, n_sq, n_cl = lax.axis_size("dp"), lax.axis_size("sq"), lax.axis_size("cl")
    dp, zi, cl = lax.axis_index("dp"), lax.axis_index("sq"), lax.axis_index("cl")
    nl, bl, width = tokens.shape
    rows = nl * bl
    n_ctx = n_sq * n_cl
    length = bl * n_ctx
    n_all = n_dp * n_ctx
    tp = n_cl * n_dp
    experts = n_ctx
    expert = zi * n_cl + cl
    capacity = max(2, (5 * bl * TOPK + 4 * experts - 1) // (4 * experts))
    ff = down_weight.shape[1]
    heads = H // tp
    hw = heads * HD
    kvw = 2 * HD // n_dp
    pack = hw + kvw
    score_scale = HD ** (-0.5)
    shard = width // n_all

    hit = jnp.any(
        routes[:, :, :, None] == jnp.arange(experts, dtype=jnp.int32), axis=2
    ).astype(bf16)
    below = jnp.tril(jnp.ones((bl, bl), bf16), -1)
    earlier = jnp.einsum("pq,jqe->jpe", below, hit, preferred_element_type=f32)
    codes = jnp.where(hit > 0, jnp.minimum(earlier + 1.0, capacity + 1.0), 0.0).astype(bf16)
    codes = jnp.pad(codes, ((0, 0), (0, 0), (0, 128 - experts)))

    small = jnp.concatenate(
        [router_weight.T.reshape(-1), norm_gains.reshape(-1)]
    )
    n_small = small.shape[0]
    n_router = experts * shard
    small = jnp.pad(small, (0, -n_small % 128)).reshape(-1, 128)
    kv_weight = jnp.concatenate(
        [k_weight.reshape(shard, n_cl, HD), v_weight.reshape(shard, n_cl, HD)], axis=-1
    )
    packed = jnp.concatenate(
        [
            q_weight.reshape(shard, n_cl, n_dp, hw),
            kv_weight.reshape(shard, n_cl, n_dp, kvw),
        ],
        axis=-1,
    )
    packed = jnp.transpose(packed, (1, 2, 0, 3)).reshape(tp, shard, pack)
    packed = lax.all_to_all(packed, ("cl", "dp"), split_axis=0, concat_axis=0, tiled=True)
    packed = jnp.transpose(packed.reshape(n_cl, n_dp, shard, pack), (1, 0, 2, 3))
    gu_full = dp_gather(gate_up_weight[0]).reshape(width, 2 * ff)
    down_full = jnp.concatenate(list(dp_gather(down_weight[0])), axis=1)

    packed, small = tie(packed, small)
    small = every_gather(small)
    qkv_w = jnp.zeros((n_dp, n_sq, n_cl, shard, pack), bf16)
    rank = cl * n_dp + dp
    qkv_pieces = [packed, shift(packed, 1)]
    inputs_low = to_sequence(tokens).reshape(rows, width)
    upstream_low = jnp.concatenate([cotangent, codes], axis=-1)
    qkv_pieces[1], inputs_low = tie(qkv_pieces[1], inputs_low)
    inputs = inputs_low.astype(f32)
    inputs_all = spread(inputs_low)
    for _ in range(2, n_sq - 1):
        qkv_pieces.append(shift(qkv_pieces[-1], 1))
    qkv_pieces[-1], inputs_all, o_weight, small = tie(
        qkv_pieces[-1], inputs_all, o_weight, small
    )
    small = small.reshape(n_all, -1)
    router_t = small[:, :n_router].reshape(n_all, experts, shard)
    router_t = jnp.transpose(router_t, (1, 0, 2)).reshape(experts, width)
    gains = small[:, n_router:n_small].reshape(-1).astype(f32)
    attn_gain = gains[:width]
    ffn_gain = gains[width : 2 * width]
    q_gain = gains[2 * width : 2 * width + HD]
    k_gain = gains[2 * width + HD :]
    qkv_pieces.append(shift(qkv_pieces[-1], 1))
    qkv_pieces[-1], gu_full, down_full, upstream_low = tie(
        qkv_pieces[-1], gu_full, down_full, upstream_low
    )
    upstream_low = to_sequence(upstream_low).reshape(rows, -1)
    upstream = upstream_low[:, :width].astype(f32)
    own_codes = upstream_low[:, width : width + experts].astype(f32)
    o_mine = lax.ppermute(o_weight, ("dp", "sq", "cl"), head_pairs())
    inputs_all = dp_rows(jnp.concatenate(inputs_all)).reshape(length, width).astype(f32)

    for t, piece in enumerate(qkv_pieces):
        qkv_w = lax.dynamic_update_index_in_dim(qkv_w, piece, (zi - t) % n_sq, 1)
    qkv_w = qkv_w.reshape(width, pack)

    order = jnp.array([[0, 1, 2, 3], [0, 2, 1, 3]], jnp.int32)
    chip_of = order ^ cl
    hb = nl // 2
    block_of = (zi - jnp.arange(nl).reshape(2, hb)) % nl
    d_ids = (jnp.arange(n_dp) ^ dp)[:, None, None, None]
    block_ids = (d_ids * nl + block_of[None, :, None, :]) * n_cl + chip_of[None, :, :, None]
    positions = block_ids[..., None] * bl + jnp.arange(bl)
    positions = positions.reshape(length).astype(jnp.int32)
    segments = take(dp_gather(segment_ids).reshape(n_dp * nl, length), zi)
    segments = segments.reshape(1, n_dp * nl * n_cl, bl)
    found = block_ids.reshape(-1, 1, 1) == jnp.arange(n_dp * nl * n_cl)[None, :, None]
    segments = jnp.sum(jnp.where(found, segments, 0), axis=1).reshape(length)
    cosine, sine_table = rope_tables(positions, HD)
    cosine, sine_table = cosine[:, None, :], sine_table[:, None, :]

    first_scale = rms_scale(inputs)
    normed_all = (inputs_all * rms_scale(inputs_all) * attn_gain).astype(bf16)
    proj = dot(normed_all, qkv_w)
    q_proj = proj[:, :hw].reshape(length, heads, HD)
    kv_proj = dp_columns(proj[:, hw:].reshape(n_dp, -1, kvw)).reshape(n_dp, length, kvw)
    kv_proj = jnp.concatenate(list(kv_proj), axis=-1)
    k_proj = kv_proj[:, None, :HD]
    values = kv_proj[:, HD:].astype(bf16)
    q_scale = rms_scale(q_proj)
    k_scale = rms_scale(k_proj)
    queries = rotate(q_proj * q_scale * q_gain, cosine, sine_table).astype(bf16)
    keys = rotate(k_proj * k_scale * k_gain, cosine, sine_table).astype(bf16)[:, 0]
    queries, o_mine = tie(queries, o_mine)
    o_pieces = [o_mine, shift(o_mine, 1)]
    values, o_pieces[1] = tie(values, o_pieces[1])
    for _ in range(2, n_sq):
        o_pieces.append(shift(o_pieces[-1], 1))
    allowed = (positions[None, :] <= positions[:, None]) & (
        segments[None, :] == segments[:, None]
    )
    scores = jnp.einsum("qhd,kd->hqk", queries, keys, preferred_element_type=f32) * score_scale
    scores = jnp.where(allowed[None], scores, neg_big)
    terms = jnp.exp(scores - jnp.max(scores, axis=-1, keepdims=True))
    probs = terms / jnp.sum(terms, axis=-1, keepdims=True)
    prob_low = probs.astype(bf16)
    attended = jnp.einsum("hqk,kd->qhd", prob_low, values, preferred_element_type=f32)
    attended = attended.reshape(length, hw).astype(bf16)
    attended, o_pieces[2] = tie(attended, o_pieces[2])
    o_full = jnp.zeros((n_sq,) + o_weight.shape, bf16)
    for t, piece in enumerate(o_pieces):
        o_full = lax.dynamic_update_index_in_dim(o_full, piece, (zi - t - rank) % n_sq, 0)
    o_full = o_full.reshape(hw, width)
    mixed = [dot(attended_m, o_full) for attended_m in attended.reshape(n_dp, -1, hw)]
    mixed = fold(dp_fold(mixed).reshape(2, n_cl, rows // 2, width)).reshape(rows, width)
    middle = inputs + mixed
    second_scale = rms_scale(middle)
    hidden = (middle * second_scale * ffn_gain).astype(bf16)
    logits = dot_nt(hidden, router_t)
    routed = own_codes > 0
    top = jnp.max(jnp.where(routed, logits, neg_big), axis=-1, keepdims=True)
    gate_terms = jnp.where(routed, jnp.exp(logits - top), 0.0)
    gates = gate_terms / jnp.sum(gate_terms, axis=-1, keepdims=True)
    gates_high = gates.astype(bf16)
    gates_low = (gates - gates_high.astype(f32)).astype(bf16)
    extra = jnp.concatenate([gates_high, gates_low, own_codes.astype(bf16)], axis=-1)
    extra = jnp.pad(extra, ((0, 0), (0, 128 - 3 * experts)))
    hidden_wide = jnp.concatenate([hidden, upstream_low[:, :width], extra], axis=-1)

    lanes = jnp.arange(128)
    half = rows // 2
    n_slot = n_cl * hb * capacity
    code_pick = jnp.broadcast_to(lanes == 2 * experts + expert, (8, 128)).astype(bf16)
    pick = (lanes == expert) | (lanes == experts + expert)

    def push(chosen, v):
        v = v.reshape(chosen.shape[:2] + (-1,))
        got = jnp.einsum("grt,grd->gtd", chosen, v, preferred_element_type=f32)
        return got.astype(bf16)

    per = 2
    n_chunk = n_sq // per
    ins, actives, out_grads, gu_grads, backs = [], [], [], [], []
    turns = list(range(1, n_sq)) + [0]
    arrived = [None] * n_sq
    moving, arrived[0] = tie(shift(hidden_wide, 1), spread(hidden_wide))
    for t in range(1, n_sq):
        arrived[t] = spread(moving)
        if t + 1 < n_sq:
            moving = shift(moving, 1)
    for chunk in range(n_chunk):
        pieces = sum([arrived[t] for t in turns[chunk * per : (chunk + 1) * per]], [])
        expert_in, grad_slot, gate_lanes, chosen = pull_pieces(
            code_pick, pieces, 2 * per, capacity, width
        )
        gate_slot = jnp.sum(
            jnp.where(pick, gate_lanes.astype(f32), 0.0), axis=-1, keepdims=True
        )
        grad_slot = grad_slot.astype(f32)
        gate_up = dot(expert_in, gu_full)
        gate_part, up_part = gate_up[:, :ff], gate_up[:, ff:]
        sigmoid_gate = jax.nn.sigmoid(gate_part)
        activated = (gate_part * sigmoid_gate * up_part).astype(bf16)
        if chunk:
            activated, back_first = tie(activated, back_first)
            backs += list(fold_last(back_first))
        expert_out = dot(activated, down_full).astype(bf16)
        out_wide = expert_out.astype(f32)
        pair_grad = jnp.sum(grad_slot * out_wide, axis=-1, keepdims=True)
        out_grad = (gate_slot * grad_slot).astype(bf16)
        act_grad = dot_nt(out_grad, down_full)
        gate_back = act_grad * up_part * sigmoid_gate * (1.0 + gate_part * (1.0 - sigmoid_gate))
        up_back = act_grad * gate_part * sigmoid_gate
        gu_grad = jnp.concatenate([gate_back, up_back], axis=-1).astype(bf16)
        if chunk:
            gu_grad, backs = tie(gu_grad, backs)
        row_grad = dot_nt(gu_grad, gu_full).astype(bf16)
        pair_high = pair_grad.astype(bf16)
        pair_low = (pair_grad - pair_high.astype(f32)).astype(bf16)
        pair_extra = jnp.where(
            lanes == expert, pair_high, jnp.where(lanes == experts + expert, pair_low, 0)
        ).astype(bf16)
        moe = (gate_slot * out_wide).astype(bf16)
        back = push(chosen, jnp.concatenate([row_grad, moe, pair_extra], axis=-1))
        if chunk + 1 < n_chunk:
            code_pick, back = tie(code_pick, back)
        back_first = fold_first(back.reshape(per, 2, n_cl, half, -1))
        ins.append(expert_in)
        actives.append(activated)
        out_grads.append(out_grad)
        gu_grads.append(gu_grad)
    gu_grad = jnp.concatenate(gu_grads)
    activated = jnp.concatenate(actives)

    def columns(parts, m):
        size = width // n_dp
        at = (dp ^ m) * size
        return jnp.concatenate([lax.dynamic_slice_in_dim(v, at, size, 1) for v in parts])

    gu_parts = [dot_tn(columns(ins, m), gu_grad) for m in range(n_dp)]
    down_parts = [dot_tn(activated, columns(out_grads, m)) for m in range(n_dp)]
    back_first, gu_parts, down_parts = tie(back_first, gu_parts, down_parts)
    backs = [v.reshape(rows, -1) for v in backs + list(fold_last(back_first))]
    back = ring_scatter(backs[-1:] + backs[:-1]).astype(bf16).astype(f32)
    output = (middle + back[:, width : 2 * width]).astype(bf16)

    pair_own = back[:, 2 * width :]
    pair_own = pair_own[:, :experts] + pair_own[:, experts : 2 * experts]
    chosen_grad = gates * (pair_own - jnp.sum(gates * pair_own, axis=-1, keepdims=True))
    logit_grad = chosen_grad.astype(bf16)
    hidden_grad = back[:, :width] + dot(logit_grad, router_t)
    router_grad = dot_tn(logit_grad, hidden)
    ffn_gain_grad = jnp.sum(hidden_grad * middle * second_scale, axis=0)
    middle_grad = upstream + norm_back(middle, second_scale, ffn_gain, hidden_grad)

    middle_low = dp_rows(jnp.concatenate(spread(middle_grad.astype(bf16)))).reshape(length, width)
    output = from_sequence(output.reshape(nl, bl, width))
    middle_low, output = tie(middle_low, output)
    o_grad = dot_tn(attended, middle_low).reshape(n_sq, -1, width)
    attended_grad = dot_nt(middle_low, o_full).astype(bf16).reshape(length, heads, HD)
    attended_grad, o_grad = tie(attended_grad, o_grad)
    o_parts = [take(o_grad, (zi - t - rank) % n_sq) for t in range(n_sq)]
    o_got = [shift(o_parts[t].astype(bf16), -t) for t in range(1, n_sq)]
    prob_grad = jnp.einsum("qhd,kd->hqk", attended_grad, values, preferred_element_type=f32)
    inner_sum = jnp.sum(probs * prob_grad, axis=-1, keepdims=True)
    score_grad = (probs * (prob_grad - inner_sum)).astype(bf16)
    value_part = jnp.einsum("hqk,qhd->kd", prob_low, attended_grad, preferred_element_type=f32)
    key_part = (
        jnp.einsum("hqk,qhd->kd", score_grad, queries, preferred_element_type=f32) * score_scale
    )
    query_grad = (
        jnp.einsum("hqk,kd->qhd", score_grad, keys, preferred_element_type=f32) * score_scale
    )
    kv_sum = jnp.concatenate([key_part, value_part], axis=-1).reshape(n_dp, -1, 2 * HD)
    kv_sum, o_got[:1] = tie(kv_sum, o_got[:1])
    kv_sum = dp_sum(kv_sum).reshape(length, 2 * HD)
    key_rot_grad = rotate_back(kv_sum[:, None, :HD], cosine, sine_table)
    k_gain_grad = jnp.sum(key_rot_grad * k_proj * k_scale, axis=(0, 1))
    k_gain_grad = jnp.where(dp == 0, k_gain_grad, 0.0)
    k_low = norm_back(k_proj, k_scale, k_gain, key_rot_grad)[:, 0].astype(bf16)
    kv_low = jnp.concatenate([k_low, kv_sum[:, HD:].astype(bf16)], axis=-1)
    kv_low = lax.dynamic_slice_in_dim(kv_low, dp * kvw, kvw, 1)
    query_rot_grad = rotate_back(query_grad, cosine, sine_table)
    q_gain_grad = jnp.sum(query_rot_grad * q_proj * q_scale, axis=(0, 1))
    q_low = norm_back(q_proj, q_scale, q_gain, query_rot_grad).reshape(length, hw).astype(bf16)
    qkv_low = jnp.concatenate([q_low, kv_low], axis=-1)
    qkv_low, gu_parts, down_parts = tie(qkv_low, gu_parts, down_parts)
    gu_share, down_share = dp_fold(gu_parts), dp_fold(down_parts)
    w_grad = dot_tn(qkv_low, normed_all)
    size = n_cl * shard

    def w_part(t):
        first = ((zi - t) % n_sq) * size
        parts = [
            lax.dynamic_slice_in_dim(w_grad, m * n_sq * size + first, size, 1)
            for m in range(n_dp)
        ]
        return jnp.concatenate(parts)

    w_got = [shift(w_part(t).astype(bf16), -t) for t in range(1, n_sq)]
    normed_grad = [dot_nt(low_m, qkv_w) for low_m in qkv_low.reshape(n_dp, -1, pack)]
    normed_grad, o_got[1:] = tie(normed_grad, o_got[1:])
    o_got = o_parts[0].astype(f32) + sum(v.astype(f32) for v in o_got)
    o_share = lax.ppermute(
        o_got.astype(bf16), ("dp", "sq", "cl"), [(b, a) for a, b in head_pairs()]
    )
    normed_first = fold_first(dp_fold(normed_grad).reshape(1, 2, n_cl, rows // 2, width))
    normed_grad = fold_last(normed_first).reshape(rows, width)
    normed_grad, w_got[:1], gu_share, down_share = tie(
        normed_grad, w_got[:1], gu_share, down_share
    )
    attn_gain_grad = jnp.sum(normed_grad * inputs * first_scale, axis=0)
    input_grad = middle_grad + norm_back(inputs, first_scale, attn_gain, normed_grad)
    input_grad = from_sequence(input_grad.astype(bf16).reshape(nl, bl, width))

    gain_grads = jnp.concatenate([attn_gain_grad, ffn_gain_grad, q_gain_grad, k_gain_grad])
    router_grad = jnp.transpose(router_grad.reshape(experts, n_all, shard), (1, 0, 2))
    small_grad = jnp.concatenate(
        [router_grad.reshape(n_all, n_router), gain_grads.reshape(n_all, -1)], axis=-1
    )
    small_grad = jnp.pad(small_grad, ((0, 0), (0, -n_small % 128))).reshape(n_all, -1, 128)
    small_grad = every_scatter(small_grad).reshape(-1)
    w_got, small_grad = tie(w_got, small_grad)
    w_got = w_part(0) + sum(v.astype(f32) for v in w_got)
    w_got, o_share = tie(w_got, o_share)
    o_share = o_share.astype(f32)
    w_grad = w_got.astype(bf16).reshape(n_dp, pack, n_cl, shard)
    w_grad = jnp.transpose(w_grad, (2, 0, 3, 1)).reshape(tp, shard, pack)
    w_grad = lax.all_to_all(w_grad, ("cl", "dp"), split_axis=0, concat_axis=0, tiled=True)
    w_grad = jnp.transpose(w_grad.reshape(n_cl, n_dp, shard, pack), (2, 0, 1, 3)).astype(f32)
    q_share = w_grad[..., :hw].reshape(shard, -1)
    kv_share = w_grad[..., hw:].reshape(shard, n_cl, 2 * HD)
    k_share = kv_share[..., :HD].reshape(shard, -1)
    v_share = kv_share[..., HD:].reshape(shard, -1)

    router_share = small_grad[:n_router].reshape(experts, shard).T
    gains_share = small_grad[n_router:n_small]
    return (
        output,
        input_grad,
        q_share,
        k_share,
        v_share,
        o_share,
        router_share,
        gains_share,
        gu_share[None],
        down_share[None],
    )


def solution(mesh):
    n_dp, n_ctx = mesh.devices.shape
    n_cl = KV
    fine = Mesh(mesh.devices.reshape(n_dp, n_ctx // n_cl, n_cl), ("dp", "sq", "cl"))
    ctx = ("sq", "cl")
    every = ("dp", "sq", "cl")
    rows = P("dp", ctx, None)
    placed = (
        rows,
        P("dp", None),
        rows,
        rows,
        P(every, None),
        P(every, None),
        P(every, None),
        P(every, None),
        P(every, None),
        P(every),
        P(ctx, "dp", None),
        P(ctx, None, "dp"),
    )
    return jax.shard_map(
        on_device,
        mesh=fine,
        in_specs=placed,
        out_specs=(
            rows,
            rows,
            P(every, None),
            P(every, None),
            P(every, None),
            P(every, None),
            P(every, None),
            P(every),
            P(ctx, "dp", None),
            P(ctx, None, "dp"),
        ),
        check_vma=False,
    )
```

```python
import jax
import jax.numpy as jnp
from jax import lax
from jax.experimental import pallas as pl
from jax.sharding import Mesh, PartitionSpec as P

H = 32
KV = 4
HD = 128
TOPK = 8
BLOCK = 64

eps_norm = 1e-06
rope_base = 1000000.0
neg_big = -1e30
f32 = jnp.float32
bf16 = jnp.bfloat16


def tie(*v):
    return lax.optimization_barrier(v)


def rms_scale(operand):
    return lax.rsqrt(jnp.mean(operand * operand, axis=-1, keepdims=True) + eps_norm)


def norm_back(operand, scale_rows, gain_vec, upstream):
    weighted = gain_vec * upstream
    inner_mean = jnp.mean(operand * weighted, axis=-1, keepdims=True)
    return scale_rows * weighted - operand * scale_rows * scale_rows * scale_rows * inner_mean


def rope_tables(positions, head_size):
    frequency = rope_base ** (-(jnp.arange(head_size // 2, dtype=f32) * 2.0 / head_size))
    angles = positions.astype(f32)[:, None] * frequency[None, :]
    angles = jnp.concatenate([angles, angles], axis=-1)
    return (jnp.cos(angles), jnp.sin(angles))


def rotate(operand, cosine, sine_table):
    half_width = operand.shape[-1] // 2
    turned = jnp.concatenate([-operand[..., half_width:], operand[..., :half_width]], axis=-1)
    return operand * cosine + turned * sine_table


def rotate_back(upstream, cosine, sine_table):
    shifted = upstream * sine_table
    half_width = upstream.shape[-1] // 2
    return upstream * cosine + jnp.concatenate(
        [shifted[..., half_width:], -shifted[..., :half_width]], axis=-1
    )


def dot(a, b):
    return jnp.dot(a, b, preferred_element_type=f32)


def dot_nt(a, b):
    return lax.dot_general(a, b, (((1,), (1,)), ((), ())), preferred_element_type=f32)


def dot_tn(a, b):
    return lax.dot_general(a, b, (((0,), (0,)), ((), ())), preferred_element_type=f32)


def take(v, index, axis=0):
    return lax.dynamic_index_in_dim(v, index, axis, keepdims=False)


def flip(v, axis, bit):
    n = lax.axis_size(axis)
    return lax.ppermute(v, axis, [(i, i ^ bit) for i in range(n)])


def px(v):
    return flip(v, "cl", 1)


def py(v):
    return flip(v, "cl", 2)


def shift(v, by):
    n = lax.axis_size("sq")
    return lax.ppermute(v, "sq", [(i, (i + by) % n) for i in range(n)])


def bits_of(axis):
    n, bit, out = lax.axis_size(axis), 1, []
    while bit < n:
        out.append(bit)
        bit *= 2
    return out


def every_gather(v):
    n = lax.axis_size("dp") * lax.axis_size("sq") * lax.axis_size("cl")
    v = jnp.broadcast_to(v[None], (n,) + v.shape)
    return lax.all_to_all(v, ("dp", "sq", "cl"), split_axis=0, concat_axis=0, tiled=True)


def every_scatter(v):
    v = lax.all_to_all(v, ("dp", "sq", "cl"), split_axis=0, concat_axis=0, tiled=True)
    return jnp.sum(v, axis=0)


def xor_groups(v, bit):
    rest = v.shape[1:]
    v = v.reshape((-1, 2, bit) + rest)
    return jnp.concatenate([v[:, 1:], v[:, :1]], axis=1).reshape((-1,) + rest)


def dp_gather(v):
    v = v[None]
    index = lax.axis_index("dp")
    for bit in bits_of("dp"):
        other = flip(v, "dp", bit)
        upper = (index & bit) != 0
        v = jnp.concatenate([jnp.where(upper, other, v), jnp.where(upper, v, other)], axis=0)
    return v


def dp_columns(v):
    v = v[None]
    index = lax.axis_index("dp")
    for bit in bits_of("dp"):
        other = flip(v, "dp", bit)
        other = jnp.swapaxes(xor_groups(jnp.swapaxes(other, 0, 1), bit), 0, 1)
        upper = (index & bit) != 0
        v = jnp.concatenate([jnp.where(upper, other, v), jnp.where(upper, v, other)], axis=0)
    return v


def dp_rows(v):
    v = v[None]
    for bit in bits_of("dp"):
        v = jnp.concatenate([v, flip(v, "dp", bit)], axis=0)
    return v


def dp_fold(parts):
    for bit in reversed(bits_of("dp")):
        parts = [
            parts[m].astype(f32) + flip(parts[m + bit].astype(bf16), "dp", bit).astype(f32)
            for m in range(bit)
        ]
    return parts[0]


def dp_sum(v):
    for bit in bits_of("dp"):
        v = v + xor_groups(flip(v.astype(bf16), "dp", bit), bit).astype(f32)
    return v


def to_sequence(v):
    nl, n_dp, n_sq = v.shape[0], lax.axis_size("dp"), lax.axis_size("sq")
    zi = lax.axis_index("sq")
    got = []
    for m in range(nl):
        pairs = [
            (d * n_sq + z, (z // nl) * n_sq + nl * d + (m + z) % nl)
            for d in range(n_dp)
            for z in range(n_sq)
        ]
        got.append(lax.ppermute(take(v, (m + zi) % nl), ("dp", "sq"), pairs))
    return jnp.stack(got)


def from_sequence(v):
    nl, n_dp, n_sq = v.shape[0], lax.axis_size("dp"), lax.axis_size("sq")
    zi = lax.axis_index("sq")
    got = []
    for m in range(nl):
        pairs = [
            ((z // nl) * n_sq + nl * d + (m + z) % nl, d * n_sq + z)
            for d in range(n_dp)
            for z in range(n_sq)
        ]
        got.append(lax.ppermute(v[m], ("dp", "sq"), pairs))
    got = jnp.stack(got)
    return jnp.stack([take(got, (j - zi) % nl) for j in range(nl)])


def head_pairs():
    n_dp, n_sq, n_cl = lax.axis_size("dp"), lax.axis_size("sq"), lax.axis_size("cl")
    pairs = []
    for f in range(n_dp * n_sq * n_cl):
        r, q = f // n_sq, f % n_sq
        pairs.append((f, ((r % n_dp) * n_sq + (q + r) % n_sq) * n_cl + r // n_dp))
    return pairs


def spread(v):
    h = v.shape[0] // 2
    a, b = v[:h], v[h:]
    a1, b1 = px(a), py(b)
    a2, b2 = py(a), px(b)
    a3, b3 = py(a1), px(b1)
    return [a, a1, a2, a3, b, b1, b2, b3]


def fold_first(v):
    ra, rb = py(v[:, 0, 2:].astype(bf16)), px(v[:, 1, 2:].astype(bf16))
    return v[:, :, :2], ra, rb


def fold_last(first):
    v, ra, rb = first
    a = v[:, 0].astype(f32) + ra.astype(f32)
    b = v[:, 1].astype(f32) + rb.astype(f32)
    a0 = a[:, 0] + px(a[:, 1].astype(bf16)).astype(f32)
    b0 = b[:, 0] + py(b[:, 1].astype(bf16)).astype(f32)
    return jnp.stack([a0, b0], axis=1)


def fold(v):
    return fold_last(fold_first(v[None]))[0]


def ring_gather(v):
    got = [v]
    for _ in range(lax.axis_size("sq") - 1):
        got.append(shift(got[-1], 1))
    return got


def ring_scatter(parts):
    moving = parts[1]
    for t in list(range(2, len(parts))) + [0]:
        got = shift(moving.astype(bf16), 1)
        moving = parts[t].astype(f32) + got.astype(f32)
    return moving


def pull_kernel(pick, *refs):
    *pieces, main, grads, tail, select = refs
    groups, slots, depth = select.shape
    n = len(pieces) // groups
    width = main.shape[-1]
    capacity = slots // (depth // BLOCK)
    place = lax.broadcasted_iota(jnp.int32, (1, depth), 1) // BLOCK
    place = (place * 128).astype(f32)
    ids = lax.broadcasted_iota(jnp.int32, (slots, 1), 0)
    ids = ((ids // capacity) * 128 + ids % capacity + 1).astype(f32)
    for g in range(groups):
        mine = pieces[g * n : (g + 1) * n]
        last = jnp.concatenate([piece[:, pl.ds(2 * width, 128)] for piece in mine], axis=0)
        code = dot_nt(pick[...], last)[:1]
        kept = (code > 0.0) & (code <= capacity)
        code = jnp.where(kept, code + place, -1.0)
        chosen = jnp.where(code == ids, 1.0, 0.0).astype(bf16)
        select[g] = chosen
        at = pl.ds(g * slots, slots)
        for out, first in ((main, 0), (grads, width)):
            rows = [piece[:, pl.ds(first, width)] for piece in mine]
            rows = jnp.concatenate(rows, axis=0)
            out[at, :] = dot(chosen, rows).astype(bf16)
        tail[at, :] = dot(chosen, last).astype(bf16)


def pull_pieces(pick, pieces, groups, capacity, width):
    depth = len(pieces) // groups * pieces[0].shape[0]
    slots = depth // BLOCK * capacity
    shapes = [(groups * slots, width), (groups * slots, width), (groups * slots, 128)]
    shapes.append((groups, slots, depth))
    return pl.pallas_call(
        pull_kernel,
        out_shape=tuple(jax.ShapeDtypeStruct(shape, bf16) for shape in shapes),
        name="pull",
    )(pick, *pieces)


def on_device(
    tokens,
    segment_ids,
    routes,
    cotangent,
    q_weight,
    k_weight,
    v_weight,
    o_weight,
    router_weight,
    norm_gains,
    gate_up_weight,
    down_weight,
):
    n_dp, n_sq, n_cl = lax.axis_size("dp"), lax.axis_size("sq"), lax.axis_size("cl")
    dp, zi, cl = lax.axis_index("dp"), lax.axis_index("sq"), lax.axis_index("cl")
    nl, bl, width = tokens.shape
    rows = nl * bl
    n_ctx = n_sq * n_cl
    length = bl * n_ctx
    n_all = n_dp * n_ctx
    tp = n_cl * n_dp
    experts = n_ctx
    expert = zi * n_cl + cl
    capacity = max(2, (5 * bl * TOPK + 4 * experts - 1) // (4 * experts))
    ff = down_weight.shape[1]
    heads = H // tp
    hw = heads * HD
    kvw = 2 * HD // n_dp
    pack = hw + kvw
    score_scale = HD ** (-0.5)
    shard = width // n_all

    hit = jnp.any(
        routes[:, :, :, None] == jnp.arange(experts, dtype=jnp.int32), axis=2
    ).astype(bf16)
    below = jnp.tril(jnp.ones((bl, bl), bf16), -1)
    earlier = jnp.einsum("pq,jqe->jpe", below, hit, preferred_element_type=f32)
    codes = jnp.where(hit > 0, jnp.minimum(earlier + 1.0, capacity + 1.0), 0.0).astype(bf16)
    codes = jnp.pad(codes, ((0, 0), (0, 0), (0, 128 - experts)))

    small = jnp.concatenate(
        [router_weight.T.reshape(-1), norm_gains.reshape(-1)]
    )
    n_small = small.shape[0]
    n_router = experts * shard
    small = jnp.pad(small, (0, -n_small % 128)).reshape(-1, 128)
    kv_weight = jnp.concatenate(
        [k_weight.reshape(shard, n_cl, HD), v_weight.reshape(shard, n_cl, HD)], axis=-1
    )
    packed = jnp.concatenate(
        [
            q_weight.reshape(shard, n_cl, n_dp, hw),
            kv_weight.reshape(shard, n_cl, n_dp, kvw),
        ],
        axis=-1,
    )
    packed = jnp.transpose(packed, (1, 2, 0, 3)).reshape(tp, shard, pack)
    packed = lax.all_to_all(packed, ("cl", "dp"), split_axis=0, concat_axis=0, tiled=True)
    packed = jnp.transpose(packed.reshape(n_cl, n_dp, shard, pack), (1, 0, 2, 3))
    gu_full = dp_gather(gate_up_weight[0]).reshape(width, 2 * ff)
    down_full = jnp.concatenate(list(dp_gather(down_weight[0])), axis=1)

    packed, small = tie(packed, small)
    small = every_gather(small)
    qkv_w = jnp.zeros((n_dp, n_sq, n_cl, shard, pack), bf16)
    rank = cl * n_dp + dp
    qkv_pieces = [packed, shift(packed, 1)]
    inputs_low = to_sequence(tokens).reshape(rows, width)
    upstream_low = jnp.concatenate([cotangent, codes], axis=-1)
    qkv_pieces[1], inputs_low = tie(qkv_pieces[1], inputs_low)
    inputs = inputs_low.astype(f32)
    inputs_all = spread(inputs_low)
    for _ in range(2, n_sq - 1):
        qkv_pieces.append(shift(qkv_pieces[-1], 1))
    qkv_pieces[-1], inputs_all, o_weight, small = tie(
        qkv_pieces[-1], inputs_all, o_weight, small
    )
    small = small.reshape(n_all, -1)
    router_t = small[:, :n_router].reshape(n_all, experts, shard)
    router_t = jnp.transpose(router_t, (1, 0, 2)).reshape(experts, width)
    gains = small[:, n_router:n_small].reshape(-1).astype(f32)
    attn_gain = gains[:width]
    ffn_gain = gains[width : 2 * width]
    q_gain = gains[2 * width : 2 * width + HD]
    k_gain = gains[2 * width + HD :]
    qkv_pieces.append(shift(qkv_pieces[-1], 1))
    qkv_pieces[-1], gu_full, down_full, upstream_low = tie(
        qkv_pieces[-1], gu_full, down_full, upstream_low
    )
    upstream_low = to_sequence(upstream_low).reshape(rows, -1)
    upstream = upstream_low[:, :width].astype(f32)
    own_codes = upstream_low[:, width : width + experts].astype(f32)
    o_mine = lax.ppermute(o_weight, ("dp", "sq", "cl"), head_pairs())
    inputs_all = dp_rows(jnp.concatenate(inputs_all)).reshape(length, width).astype(f32)

    for t, piece in enumerate(qkv_pieces):
        qkv_w = lax.dynamic_update_index_in_dim(qkv_w, piece, (zi - t) % n_sq, 1)
    qkv_w = qkv_w.reshape(width, pack)

    order = jnp.array([[0, 1, 2, 3], [0, 2, 1, 3]], jnp.int32)
    chip_of = order ^ cl
    hb = nl // 2
    block_of = (zi - jnp.arange(nl).reshape(2, hb)) % nl
    d_ids = (jnp.arange(n_dp) ^ dp)[:, None, None, None]
    block_ids = (d_ids * nl + block_of[None, :, None, :]) * n_cl + chip_of[None, :, :, None]
    positions = block_ids[..., None] * bl + jnp.arange(bl)
    positions = positions.reshape(length).astype(jnp.int32)
    segments = take(dp_gather(segment_ids).reshape(n_dp * nl, length), zi)
    segments = segments.reshape(1, n_dp * nl * n_cl, bl)
    found = block_ids.reshape(-1, 1, 1) == jnp.arange(n_dp * nl * n_cl)[None, :, None]
    segments = jnp.sum(jnp.where(found, segments, 0), axis=1).reshape(length)
    cosine, sine_table = rope_tables(positions, HD)
    cosine, sine_table = cosine[:, None, :], sine_table[:, None, :]

    first_scale = rms_scale(inputs)
    normed_all = (inputs_all * rms_scale(inputs_all) * attn_gain).astype(bf16)
    (normed_all,) = tie(normed_all)
    proj = dot(normed_all, qkv_w)
    q_proj = proj[:, :hw].reshape(length, heads, HD)
    kv_proj = dp_columns(proj[:, hw:].reshape(n_dp, -1, kvw)).reshape(n_dp, length, kvw)
    kv_proj = jnp.concatenate(list(kv_proj), axis=-1)
    k_proj = kv_proj[:, None, :HD]
    values = kv_proj[:, HD:].astype(bf16)
    q_scale = rms_scale(q_proj)
    k_scale = rms_scale(k_proj)
    queries = rotate(q_proj * q_scale * q_gain, cosine, sine_table).astype(bf16)
    keys = rotate(k_proj * k_scale * k_gain, cosine, sine_table).astype(bf16)[:, 0]
    queries, o_mine = tie(queries, o_mine)
    o_pieces = [o_mine, shift(o_mine, 1)]
    values, o_pieces[1] = tie(values, o_pieces[1])
    for _ in range(2, n_sq):
        o_pieces.append(shift(o_pieces[-1], 1))
    allowed = (positions[None, :] <= positions[:, None]) & (
        segments[None, :] == segments[:, None]
    )
    scores = jnp.einsum("qhd,kd->hqk", queries, keys, preferred_element_type=f32) * score_scale
    scores = jnp.where(allowed[None], scores, neg_big)
    terms = jnp.exp(scores - jnp.max(scores, axis=-1, keepdims=True))
    probs = terms / jnp.sum(terms, axis=-1, keepdims=True)
    prob_low = probs.astype(bf16)
    attended = jnp.einsum("hqk,kd->qhd", prob_low, values, preferred_element_type=f32)
    attended = attended.reshape(length, hw).astype(bf16)
    attended, o_pieces[2] = tie(attended, o_pieces[2])
    o_full = jnp.zeros((n_sq,) + o_weight.shape, bf16)
    for t, piece in enumerate(o_pieces):
        o_full = lax.dynamic_update_index_in_dim(o_full, piece, (zi - t - rank) % n_sq, 0)
    o_full = o_full.reshape(hw, width)
    mixed = [dot(attended_m, o_full) for attended_m in attended.reshape(n_dp, -1, hw)]
    mixed = fold(dp_fold(mixed).reshape(2, n_cl, rows // 2, width)).reshape(rows, width)
    middle = inputs + mixed
    second_scale = rms_scale(middle)
    hidden = (middle * second_scale * ffn_gain).astype(bf16)
    logits = dot_nt(hidden, router_t)
    routed = own_codes > 0
    top = jnp.max(jnp.where(routed, logits, neg_big), axis=-1, keepdims=True)
    gate_terms = jnp.where(routed, jnp.exp(logits - top), 0.0)
    gates = gate_terms / jnp.sum(gate_terms, axis=-1, keepdims=True)
    gates_high = gates.astype(bf16)
    gates_low = (gates - gates_high.astype(f32)).astype(bf16)
    extra = jnp.concatenate([gates_high, gates_low, own_codes.astype(bf16)], axis=-1)
    extra = jnp.pad(extra, ((0, 0), (0, 128 - 3 * experts)))
    hidden_wide = jnp.concatenate([hidden, upstream_low[:, :width], extra], axis=-1)

    lanes = jnp.arange(128)
    half = rows // 2
    n_slot = n_cl * hb * capacity
    code_pick = jnp.broadcast_to(lanes == 2 * experts + expert, (8, 128)).astype(bf16)
    pick = (lanes == expert) | (lanes == experts + expert)

    def push(chosen, v):
        v = v.reshape(chosen.shape[:2] + (-1,))
        got = jnp.einsum("grt,grd->gtd", chosen, v, preferred_element_type=f32)
        return got.astype(bf16)

    per = 2
    n_chunk = n_sq // per
    ins, actives, out_grads, gu_grads, backs = [], [], [], [], []
    turns = list(range(1, n_sq)) + [0]
    arrived = [None] * n_sq
    moving, arrived[0] = tie(shift(hidden_wide, 1), spread(hidden_wide))
    for t in range(1, n_sq):
        arrived[t] = spread(moving)
        if t + 1 < n_sq:
            moving = shift(moving, 1)
    for chunk in range(n_chunk):
        pieces = sum([arrived[t] for t in turns[chunk * per : (chunk + 1) * per]], [])
        expert_in, grad_slot, gate_lanes, chosen = pull_pieces(
            code_pick, pieces, 2 * per, capacity, width
        )
        gate_slot = jnp.sum(
            jnp.where(pick, gate_lanes.astype(f32), 0.0), axis=-1, keepdims=True
        )
        grad_slot = grad_slot.astype(f32)
        gate_up = dot(expert_in, gu_full)
        gate_part, up_part = gate_up[:, :ff], gate_up[:, ff:]
        sigmoid_gate = jax.nn.sigmoid(gate_part)
        activated = (gate_part * sigmoid_gate * up_part).astype(bf16)
        if chunk:
            activated, back_first = tie(activated, back_first)
            backs += list(fold_last(back_first))
        expert_out = dot(activated, down_full).astype(bf16)
        out_wide = expert_out.astype(f32)
        pair_grad = jnp.sum(grad_slot * out_wide, axis=-1, keepdims=True)
        out_grad = (gate_slot * grad_slot).astype(bf16)
        act_grad = dot_nt(out_grad, down_full)
        gate_back = act_grad * up_part * sigmoid_gate * (1.0 + gate_part * (1.0 - sigmoid_gate))
        up_back = act_grad * gate_part * sigmoid_gate
        gu_grad = jnp.concatenate([gate_back, up_back], axis=-1).astype(bf16)
        if chunk:
            gu_grad, backs = tie(gu_grad, backs)
        row_grad = dot_nt(gu_grad, gu_full).astype(bf16)
        pair_high = pair_grad.astype(bf16)
        pair_low = (pair_grad - pair_high.astype(f32)).astype(bf16)
        pair_extra = jnp.where(
            lanes == expert, pair_high, jnp.where(lanes == experts + expert, pair_low, 0)
        ).astype(bf16)
        moe = (gate_slot * out_wide).astype(bf16)
        back = push(chosen, jnp.concatenate([row_grad, moe, pair_extra], axis=-1))
        if chunk + 1 < n_chunk:
            code_pick, back = tie(code_pick, back)
        back_first = fold_first(back.reshape(per, 2, n_cl, half, -1))
        ins.append(expert_in)
        actives.append(activated)
        out_grads.append(out_grad)
        gu_grads.append(gu_grad)
    gu_grad = jnp.concatenate(gu_grads)
    activated = jnp.concatenate(actives)

    def columns(parts, m):
        size = width // n_dp
        at = (dp ^ m) * size
        return jnp.concatenate([lax.dynamic_slice_in_dim(v, at, size, 1) for v in parts])

    gu_parts = [dot_tn(columns(ins, m), gu_grad) for m in range(n_dp)]
    down_parts = [dot_tn(activated, columns(out_grads, m)) for m in range(n_dp)]
    back_first, gu_parts, down_parts = tie(back_first, gu_parts, down_parts)
    backs = [v.reshape(rows, -1) for v in backs + list(fold_last(back_first))]
    back = ring_scatter(backs[-1:] + backs[:-1]).astype(bf16).astype(f32)
    output = (middle + back[:, width : 2 * width]).astype(bf16)

    pair_own = back[:, 2 * width :]
    pair_own = pair_own[:, :experts] + pair_own[:, experts : 2 * experts]
    chosen_grad = gates * (pair_own - jnp.sum(gates * pair_own, axis=-1, keepdims=True))
    logit_grad = chosen_grad.astype(bf16)
    hidden_grad = back[:, :width] + dot(logit_grad, router_t)
    router_grad = dot_tn(logit_grad, hidden)
    ffn_gain_grad = jnp.sum(hidden_grad * middle * second_scale, axis=0)
    middle_grad = upstream + norm_back(middle, second_scale, ffn_gain, hidden_grad)

    middle_low = dp_rows(jnp.concatenate(spread(middle_grad.astype(bf16)))).reshape(length, width)
    output = from_sequence(output.reshape(nl, bl, width))
    middle_low, output = tie(middle_low, output)
    o_grad = dot_tn(attended, middle_low).reshape(n_sq, -1, width)
    attended_grad = dot_nt(middle_low, o_full).astype(bf16).reshape(length, heads, HD)
    attended_grad, o_grad = tie(attended_grad, o_grad)
    o_parts = [take(o_grad, (zi - t - rank) % n_sq) for t in range(n_sq)]
    o_got = [shift(o_parts[t].astype(bf16), -t) for t in range(1, n_sq)]
    prob_grad = jnp.einsum("qhd,kd->hqk", attended_grad, values, preferred_element_type=f32)
    inner_sum = jnp.sum(probs * prob_grad, axis=-1, keepdims=True)
    score_grad = (probs * (prob_grad - inner_sum)).astype(bf16)
    value_part = jnp.einsum("hqk,qhd->kd", prob_low, attended_grad, preferred_element_type=f32)
    key_part = (
        jnp.einsum("hqk,qhd->kd", score_grad, queries, preferred_element_type=f32) * score_scale
    )
    query_grad = (
        jnp.einsum("hqk,kd->qhd", score_grad, keys, preferred_element_type=f32) * score_scale
    )
    kv_sum = jnp.concatenate([key_part, value_part], axis=-1).reshape(n_dp, -1, 2 * HD)
    kv_sum, o_got[:1] = tie(kv_sum, o_got[:1])
    kv_sum = dp_sum(kv_sum).reshape(length, 2 * HD)
    key_rot_grad = rotate_back(kv_sum[:, None, :HD], cosine, sine_table)
    k_gain_grad = jnp.sum(key_rot_grad * k_proj * k_scale, axis=(0, 1))
    k_gain_grad = jnp.where(dp == 0, k_gain_grad, 0.0)
    k_low = norm_back(k_proj, k_scale, k_gain, key_rot_grad)[:, 0].astype(bf16)
    kv_low = jnp.concatenate([k_low, kv_sum[:, HD:].astype(bf16)], axis=-1)
    kv_low = lax.dynamic_slice_in_dim(kv_low, dp * kvw, kvw, 1)
    query_rot_grad = rotate_back(query_grad, cosine, sine_table)
    q_gain_grad = jnp.sum(query_rot_grad * q_proj * q_scale, axis=(0, 1))
    q_low = norm_back(q_proj, q_scale, q_gain, query_rot_grad).reshape(length, hw).astype(bf16)
    qkv_low = jnp.concatenate([q_low, kv_low], axis=-1)
    qkv_low, gu_parts, down_parts = tie(qkv_low, gu_parts, down_parts)
    gu_share, down_share = dp_fold(gu_parts), dp_fold(down_parts)
    w_grad = dot_tn(qkv_low, normed_all)
    size = n_cl * shard

    def w_part(t):
        first = ((zi - t) % n_sq) * size
        parts = [
            lax.dynamic_slice_in_dim(w_grad, m * n_sq * size + first, size, 1)
            for m in range(n_dp)
        ]
        return jnp.concatenate(parts)

    w_got = [shift(w_part(t).astype(bf16), -t) for t in range(1, n_sq)]
    normed_grad = [dot_nt(low_m, qkv_w) for low_m in qkv_low.reshape(n_dp, -1, pack)]
    normed_grad, o_got[1:] = tie(normed_grad, o_got[1:])
    o_got = o_parts[0].astype(f32) + sum(v.astype(f32) for v in o_got)
    o_share = lax.ppermute(
        o_got.astype(bf16), ("dp", "sq", "cl"), [(b, a) for a, b in head_pairs()]
    )
    normed_first = fold_first(dp_fold(normed_grad).reshape(1, 2, n_cl, rows // 2, width))
    normed_grad = fold_last(normed_first).reshape(rows, width)
    normed_grad, w_got[:1], gu_share, down_share = tie(
        normed_grad, w_got[:1], gu_share, down_share
    )
    attn_gain_grad = jnp.sum(normed_grad * inputs * first_scale, axis=0)
    input_grad = middle_grad + norm_back(inputs, first_scale, attn_gain, normed_grad)
    input_grad = from_sequence(input_grad.astype(bf16).reshape(nl, bl, width))

    gain_grads = jnp.concatenate([attn_gain_grad, ffn_gain_grad, q_gain_grad, k_gain_grad])
    router_grad = jnp.transpose(router_grad.reshape(experts, n_all, shard), (1, 0, 2))
    small_grad = jnp.concatenate(
        [router_grad.reshape(n_all, n_router), gain_grads.reshape(n_all, -1)], axis=-1
    )
    small_grad = jnp.pad(small_grad, ((0, 0), (0, -n_small % 128))).reshape(n_all, -1, 128)
    small_grad = every_scatter(small_grad).reshape(-1)
    w_got, small_grad = tie(w_got, small_grad)
    w_got = w_part(0) + sum(v.astype(f32) for v in w_got)
    w_got, o_share = tie(w_got, o_share)
    o_share = o_share.astype(f32)
    w_grad = w_got.astype(bf16).reshape(n_dp, pack, n_cl, shard)
    w_grad = jnp.transpose(w_grad, (2, 0, 3, 1)).reshape(tp, shard, pack)
    w_grad = lax.all_to_all(w_grad, ("cl", "dp"), split_axis=0, concat_axis=0, tiled=True)
    w_grad = jnp.transpose(w_grad.reshape(n_cl, n_dp, shard, pack), (2, 0, 1, 3)).astype(f32)
    q_share = w_grad[..., :hw].reshape(shard, -1)
    kv_share = w_grad[..., hw:].reshape(shard, n_cl, 2 * HD)
    k_share = kv_share[..., :HD].reshape(shard, -1)
    v_share = kv_share[..., HD:].reshape(shard, -1)

    router_share = small_grad[:n_router].reshape(experts, shard).T
    gains_share = small_grad[n_router:n_small]
    return (
        output,
        input_grad,
        q_share,
        k_share,
        v_share,
        o_share,
        router_share,
        gains_share,
        gu_share[None],
        down_share[None],
    )


def solution(mesh):
    n_dp, n_ctx = mesh.devices.shape
    n_cl = KV
    fine = Mesh(mesh.devices.reshape(n_dp, n_ctx // n_cl, n_cl), ("dp", "sq", "cl"))
    ctx = ("sq", "cl")
    every = ("dp", "sq", "cl")
    rows = P("dp", ctx, None)
    placed = (
        rows,
        P("dp", None),
        rows,
        rows,
        P(every, None),
        P(every, None),
        P(every, None),
        P(every, None),
        P(every, None),
        P(every),
        P(ctx, "dp", None),
        P(ctx, None, "dp"),
    )
    return jax.shard_map(
        on_device,
        mesh=fine,
        in_specs=placed,
        out_specs=(
            rows,
            rows,
            P(every, None),
            P(every, None),
            P(every, None),
            P(every, None),
            P(every, None),
            P(every),
            P(ctx, "dp", None),
            P(ctx, None, "dp"),
        ),
        check_vma=False,
    )
```
